256 devices in a mesh: dp: 32 (over z, y), tensor: 8 (over x, core).
Axes of the slice: x: 4, y: 4, z: 8, core: 2. Of those that a mesh axis runs over, the one named last changes fastest.
Arguments:
- layer_outs: bfloat16 [5, 32768, 4096], P(None, 'dp', 'tensor'), may hold values from -6 to 6
- avg_grads: bfloat16 [4, 32768, 4096], P(None, 'dp', 'tensor'), may hold values from -0.00051498413 to 0.00051498413
- attn_mixed: bfloat16 [32768, 4096], P('dp', 'tensor'), may hold values from -96 to 96
- dwa_coefs: float32 [4, 5], replicated, may hold values from -1.5 to 1.5
Outputs:
- coef_grad: float32 [4, 5], replicated
- proj_grad: float32 [4096, 4096], P('dp', 'tensor')
The draws below stay inside these ranges and needn't reach their ends.
All inputs are finite; a program needn't handle non-finite values.
Results may differ from the reference program's by a relative error of at most 0.0042.
Values may be sent and summed in bfloat16 or wider, within the bound.
A program may use at most 64 MiB of HBM per device.

```python
import jax
import jax.numpy as jnp
from jax import lax

D = 4096
LAYERS = 4
TOKENS = 32768


def steps_of(rng, dims, split, least, largest):
    factor_of, own = 1.0, jax.random.fold_in(rng, 6)
    for dim, blocks in split:
        heights = jnp.exp(jax.random.uniform(jax.random.fold_in(own, dim), (blocks,), jnp.float32, least / len(split), largest / len(split)))
        factor_of = factor_of * jnp.repeat(heights, dims[dim] // blocks).reshape([-1 if axis == dim else 1 for axis in range(len(dims))])
    return factor_of


def bell_draw(own_key, dims, scale, bound, split=(), kind=jnp.bfloat16):
    array = scale * jax.random.normal(own_key, dims, jnp.float32)
    if split:
        array = array * steps_of(own_key, dims, split, -0.22, 0.18)
    return jnp.clip(array, -bound, bound).astype(kind)


def setup_inputs(seed: int = 0) -> dict:
    keys = jax.random.split(jax.random.key(seed), 5)
    layer_outs = bell_draw(keys[0], (LAYERS + 1, TOKENS, D), 1.0, 6.0, ((1, 32), (2, 8)))
    avg_grads = bell_draw(keys[1], (LAYERS, TOKENS, D), (1.0 / (TOKENS * D) ** 0.5), 0.00051498413, ((1, 32), (2, 8)))
    attn_mixed = bell_draw(keys[2], (TOKENS, D), (D ** 0.5 / 4), 96.0, ((0, 32), (1, 8)))
    dwa_coefs = jnp.clip(jax.random.uniform(keys[3], (LAYERS, LAYERS + 1), jnp.float32, -1.5, 1.5), -1.5, 1.5)
    return dict(layer_outs=layer_outs, avg_grads=avg_grads, attn_mixed=attn_mixed, dwa_coefs=dwa_coefs)


def reference(layer_outs, avg_grads, attn_mixed, dwa_coefs):
    grads_flat = avg_grads.reshape(LAYERS, -1)
    outs_flat = layer_outs.reshape(LAYERS + 1, -1)
    raw = lax.dot_general(grads_flat, outs_flat, (((1,), (1,)), ((), ())), preferred_element_type=jnp.float32)
    rows = jnp.arange(LAYERS, dtype=jnp.int32)[:, None]
    cols = jnp.arange(LAYERS + 1, dtype=jnp.int32)[None, :]
    coef_grad = jnp.where(cols <= rows + 1, raw, jnp.float32(0.0))
    first = dwa_coefs[LAYERS - 2, LAYERS - 1] * avg_grads[LAYERS - 2].astype(jnp.float32)
    second = dwa_coefs[LAYERS - 1, LAYERS - 1] * avg_grads[LAYERS - 1].astype(jnp.float32)
    out_grad = (first + second).astype(jnp.bfloat16)
    proj_grad = lax.dot_general(out_grad, attn_mixed, (((0,), (0,)), ((), ())), preferred_element_type=jnp.float32)
    return coef_grad, proj_grad
```

```python
import jax
import jax.numpy as jnp
from jax import lax
from jax.experimental import pallas as pl
from jax.experimental.pallas import tpu as pltpu
from jax.sharding import PartitionSpec as P

MESH = pl.DeviceIdType.MESH
F32, BF16 = jnp.float32, jnp.bfloat16
NX, NY, NZ = 4, 4, 8
PAIRS = [(i, j) for i in range(4) for j in range(5) if j <= i + 1]


def kernel(
    co, lo_h, ag_h, at_h, coef_out, proj_out,
    lo, ag, ab, gt, pf, s1, r1, s2, r2, zs, zr, zsum, outb, cb_c, cb_x, cb_y, cb_z,
    in_sem, gd_s, gd_r, gx_s, gx_r, gf_s, gf_r, ax_s, ax_r,
    y1_s, y1_r, y2_s, y2_r, z_s, z_r, f_s, f_r, c_s, c_r,
):
    dp, tk = lax.axis_index("dp"), lax.axis_index("tensor")
    z, y = dp // NY, dp % NY
    x, c = tk // 2, tk % 2
    xg = x + 1 - 2 * (x % 2)
    xa = NX - 1 - x

    def dev(x_, y_, z_, c_):
        return (z_ * NY + y_, x_ * 2 + c_)

    def send(src, dst, send_sem, recv_sem, where):
        copy = pltpu.make_async_remote_copy(
            src_ref=src, dst_ref=dst, send_sem=send_sem, recv_sem=recv_sem,
            device_id=where, device_id_type=MESH,
        )
        copy.start()

    def arrived(ref, sem):
        pltpu.make_async_copy(ref, ref, sem).wait()

    others_x = [(x + k) % NX for k in range(1, NX)]
    others_y = [(y + k) % NY for k in range(1, NY)]
    others_z = [(z + k) % NZ for k in range(1, NZ)]

    loads = {}

    def load(name, src, dst, i):
        loads[name] = pltpu.make_async_copy(src, dst, in_sem.at[i])
        loads[name].start()

    load("ag2", ag_h.at[2], ag.at[2], 0)
    load("ag3", ag_h.at[3], ag.at[3], 1)
    load("ab0", at_h.at[:, pl.ds(0, 256)], ab.at[0], 2)
    load("ab1", at_h.at[:, pl.ds(256, 256)], ab.at[1], 3)
    load("ag0", ag_h.at[0], ag.at[0], 4)
    load("ag1", ag_h.at[1], ag.at[1], 5)
    for j in range(5):
        load(f"lo{j}", lo_h.at[j], lo.at[j], 6 + j)

    barrier = pltpu.get_barrier_semaphore()
    greeted = [dev(x, y, z, 1 - c)]
    greeted += [dev(x_, y, z, c) for x_ in others_x]
    greeted += [dev(x, y_, z, c) for y_ in others_y]
    greeted += [dev(x, y, z_, c) for z_ in others_z]
    greeted += [dev(xa, y, z_, c) for z_ in others_z]
    for where in greeted:
        pl.semaphore_signal(barrier, inc=1, device_id=where, device_id_type=MESH)

    loads["ag2"].wait()
    loads["ag3"].wait()
    c2, c3 = co[2, 3], co[3, 3]

    def out_grad(i, _):
        rows = pl.ds(pl.multiple_of(i * 256, 256), 256)
        for yy in range(NY):
            cols = pl.ds(yy * 128, 128)
            first = c2 * ag[2, rows, cols].astype(F32)
            second = c3 * ag[3, rows, cols].astype(F32)
            turned = (first + second).astype(BF16).T
            for hh in range(2):
                gt[hh, yy, c, :, rows] = turned[hh * 64 : hh * 64 + 64]
        return 0

    lax.fori_loop(0, 4, out_grad, 0)
    loads["ab0"].wait()
    loads["ab1"].wait()
    pl.semaphore_wait(barrier, len(greeted))

    for j in range(2):
        send(ab.at[j], ab.at[2 + j], ax_s.at[j], ax_r.at[j], dev(xa, y, z, c))
        send(gt.at[j, :, c], gt.at[2 + j, :, c], gx_s.at[j], gx_r.at[j], dev(xg, y, z, c))
        send(gt.at[j, :, c], gt.at[j, :, c], gd_s.at[j], gd_r.at[j], dev(x, y, z, 1 - c))

    up, down = dev(x, (y + 1) % NY, z, c), dev(x, (y + 3) % NY, z, c)

    def product(g, a):
        b = g * 4 + a

        def one(i, _):
            yc = (y + 2 + i) % NY
            term = jnp.dot(
                gt[g, yc].reshape(128, 1024), ab[a], preferred_element_type=F32
            )
            pf[b, yc] = term.reshape(8, 16, 256)
            return 0

        one(0, 0)
        far = pf[b, (y + 2) % NY].astype(BF16)
        s1[b, 0] = far[:, :, :128]
        s1[b, 1] = far[:, :, 128:]
        send(s1.at[b, 0], r1.at[b, 0], y1_s, y1_r.at[b, 0], up)
        send(s1.at[b, 1], r1.at[b, 1], y1_s, y1_r.at[b, 1], down)
        lax.fori_loop(1, NY, one, 0)

    def y_second(g, a):
        b = g * 4 + a
        arrived(r1.at[b, 0], y1_r.at[b, 0])
        yu = (y + 1) % NY
        s2[b, 0, :, :, :128] = (pf[b, yu, :, :, :128] + r1[b, 0].astype(F32)).astype(BF16)
        s2[b, 0, :, :, 128:] = pf[b, yu, :, :, 128:].astype(BF16)
        send(s2.at[b, 0], r2.at[b, 0], y2_s, y2_r.at[b, 0], up)
        arrived(r1.at[b, 1], y1_r.at[b, 1])
        yd = (y + 3) % NY
        s2[b, 1, :, :, :128] = pf[b, yd, :, :, :128].astype(BF16)
        s2[b, 1, :, :, 128:] = (pf[b, yd, :, :, 128:] + r1[b, 1].astype(F32)).astype(BF16)
        send(s2.at[b, 1], r2.at[b, 1], y2_s, y2_r.at[b, 1], down)

    def slot_of(z_, g):
        base = x + (xg - x) * (g // 2)
        return (z_ - 2 * base + 3 + NZ) % NZ, 2 * base

    def z_share(g, a):
        b = g * 4 + a
        arrived(r2.at[b, 0], y2_r.at[b, 0])
        arrived(r2.at[b, 1], y2_r.at[b, 1])
        total = pf[b, y] + r2[b, 0].astype(F32) + r2[b, 1].astype(F32)
        pf[b, y] = total
        zs[b] = total.astype(BF16)
        for k in range(1, NZ):
            there = (z + k) % NZ
            slot, _ = slot_of(there, g)
            send(zs.at[b, slot], zr.at[b, k - 1], z_s, z_r.at[b], dev(x, y, there, c))

    def to_home(g, a, own_plane):
        b = g * 4 + a
        arrived(zr.at[b], z_r.at[b])
        slot, home0 = slot_of(z, g)
        total = pf[b, y, slot]
        for k in range(NZ - 1):
            total = total + zr[b, k].astype(F32)
        zh = home0 + slot // 4
        block = (g % 2) * 4 + slot % 4
        if own_plane:

            @pl.when(zh == z)
            def _():
                outb[block, a % 2] = total

            @pl.when(zh != z)
            def _():
                zsum[b] = total
                send(zsum.at[b], outb.at[block, a % 2], f_s.at[b], f_r, dev(x, y, zh, c))

        else:
            zsum[b] = total
            send(zsum.at[b], outb.at[block, a % 2], f_s.at[b], f_r, dev(xa, y, zh, c))

    def run(fn, count, g_of, a_of, *more):
        def step(t, _):
            fn(g_of(t), a_of(t), *more)
            return 0

        lax.fori_loop(0, count, step, 0)

    first = (4, lambda t: t // 2, lambda t: t % 2)
    rows2, cols2 = (2, lambda t: 2, lambda t: t), (3, lambda t: t, lambda t: 2)
    rows3, cols3 = (3, lambda t: 3, lambda t: t), (4, lambda t: t, lambda t: 3)

    def all_to_home(shell, n):
        if shell == 0:
            run(to_home, 4, lambda t: t // 2, lambda t: t % 2, True)
        else:
            run(to_home, 2, lambda t: n, lambda t: t, True)
            run(to_home, n - 2, lambda t: n, lambda t: t + 2, False)
            run(to_home, n + 1, lambda t: t, lambda t: n, False)

    def features(j):
        arrived(gt.at[2 + j, :, c], gx_r.at[j])
        send(gt.at[2 + j, :, c], gt.at[2 + j, :, c], gf_s.at[j], gf_r.at[j], dev(x, y, z, 1 - c))
        arrived(gt.at[2 + j, :, 1 - c], gf_r.at[j])

    def coef_step(r, accs):
        rows = pl.ds(pl.multiple_of(r * 16, 16), 16)
        accs = list(accs)
        for q in range(4):
            cols = pl.ds(q * 128, 128)
            outs = [lo[j, rows, cols].astype(F32) for j in range(5)]
            grads = [ag[i, rows, cols].astype(F32) for i in range(4)]
            for n, (i, j) in enumerate(PAIRS):
                p = grads[i] * outs[j]
                accs[n] = accs[n] + (p[:8] + p[8:])
        return tuple(accs)

    def spread(buf, own, k0, targets, stage, size):
        for k, where in enumerate(targets):
            send(buf.at[own], buf.at[own], c_s.at[stage], c_r.at[stage], where)

    def settle(buf, own, stage, size):
        arrived(buf.at[pl.ds(0, size - 1)], c_r.at[stage])
        total = buf[0]
        for k in range(1, size):
            total = total + buf[k]
        return total

    def coef_local():
        for name in ["ag0", "ag1"] + [f"lo{j}" for j in range(5)]:
            loads[name].wait()
        zero = jnp.zeros((8, 128), F32)
        accs = lax.fori_loop(0, 64, coef_step, (zero,) * len(PAIRS))
        row = lax.broadcasted_iota(jnp.int32, (8, 128), 0)
        col = lax.broadcasted_iota(jnp.int32, (8, 128), 1)
        tile = zero
        for n, (i, j) in enumerate(PAIRS):
            total = jnp.sum(jnp.sum(accs[n], axis=0, keepdims=True), axis=1, keepdims=True)
            tile = jnp.where((row == i) & (col == j), jnp.broadcast_to(total, (8, 128)), tile)
        cb_c[c] = tile
        spread(cb_c, c, 0, [dev(x, y, z, 1 - c)], 0, 2)

    def coef_x():
        cb_x[x] = settle(cb_c, c, 0, 2)
        spread(cb_x, x, 0, [dev(x_, y, z, c) for x_ in others_x], 1, NX)

    def coef_y():
        cb_y[y] = settle(cb_x, x, 1, NX)
        spread(cb_y, y, 0, [dev(x, y_, z, c) for y_ in others_y], 2, NY)

    def coef_z():
        cb_z[z] = settle(cb_y, y, 2, NY)
        spread(cb_z, z, 0, [dev(x, y, z_, c) for z_ in others_z], 3, NZ)

    for j in range(2):
        arrived(gt.at[j, :, 1 - c], gd_r.at[j])
    run(product, *first)
    run(y_second, *first)
    coef_local()
    run(z_share, *first)
    coef_x()

    features(0)
    run(product, *rows2)
    arrived(ab.at[2], ax_r.at[0])
    run(product, *cols2)
    all_to_home(0, 0)
    coef_y()
    run(y_second, *rows2)
    run(y_second, *cols2)
    run(z_share, *rows2)
    run(z_share, *cols2)
    coef_z()

    features(1)
    run(product, *rows3)
    arrived(ab.at[3], ax_r.at[1])
    run(product, *cols3)
    all_to_home(1, 2)
    run(y_second, *rows3)
    run(y_second, *cols3)
    run(z_share, *rows3)
    run(z_share, *cols3)
    coef_out[...] = settle(cb_z, z, 3, NZ)[:4, :5]
    all_to_home(1, 3)

    at_home = z // 4 == x // 2

    @pl.when(at_home)
    def _():
        arrived(outb.at[pl.ds(0, 6)], f_r)

    @pl.when(jnp.logical_not(at_home))
    def _():
        arrived(outb, f_r)

    for block in range(8):
        for j in range(2):
            proj_out[pl.ds(block * 16, 16), pl.ds(j * 256, 256)] = outb[block, j]

    arrived(s1, y1_s)
    arrived(s2, y2_s)
    arrived(zr, z_s)
    for b in range(16):
        g, a = b // 4, b % 4
        if a < 2:
            slot, home0 = slot_of(z, g)

            @pl.when(home0 + slot // 4 != z)
            def _():
                arrived(zsum.at[b], f_s.at[b])

        else:
            arrived(zsum.at[b], f_s.at[b])
    arrived(cb_c.at[0], c_s.at[0])
    arrived(cb_x.at[pl.ds(0, NX - 1)], c_s.at[1])
    arrived(cb_y.at[pl.ds(0, NY - 1)], c_s.at[2])
    arrived(cb_z.at[pl.ds(0, NZ - 1)], c_s.at[3])
    for j in range(2):
        arrived(ab.at[j], ax_s.at[j])
        arrived(gt.at[j, :, c], gx_s.at[j])
        arrived(gt.at[j, :, c], gd_s.at[j])
        arrived(gt.at[2 + j, :, c], gf_s.at[j])


def local(layer_outs, avg_grads, attn_mixed, dwa_coefs):
    dma = pltpu.SemaphoreType.DMA
    anywhere = pl.BlockSpec(memory_space=pl.ANY)
    vmem = pl.BlockSpec(memory_space=pltpu.VMEM)
    return pl.pallas_call(
        kernel,
        out_shape=(
            jax.ShapeDtypeStruct((4, 5), F32),
            jax.ShapeDtypeStruct((128, 512), F32),
        ),
        in_specs=[pl.BlockSpec(memory_space=pltpu.SMEM), anywhere, anywhere, anywhere],
        out_specs=(vmem, vmem),
        scratch_shapes=[
            pltpu.VMEM((5, 1024, 512), BF16),
            pltpu.VMEM((4, 1024, 512), BF16),
            pltpu.VMEM((4, 1024, 256), BF16),
            pltpu.VMEM((4, NY, 2, 64, 1024), BF16),
            pltpu.VMEM((16, NY, 8, 16, 256), F32),
            pltpu.VMEM((16, 2, 8, 16, 128), BF16),
            pltpu.VMEM((16, 2, 8, 16, 128), BF16),
            pltpu.VMEM((16, 2, 8, 16, 256), BF16),
            pltpu.VMEM((16, 2, 8, 16, 256), BF16),
            pltpu.VMEM((16, 8, 16, 256), BF16),
            pltpu.VMEM((16, 7, 16, 256), BF16),
            pltpu.VMEM((16, 16, 256), F32),
            pltpu.VMEM((8, 2, 16, 256), F32),
            pltpu.VMEM((2, 8, 128), F32),
            pltpu.VMEM((NX, 8, 128), F32),
            pltpu.VMEM((NY, 8, 128), F32),
            pltpu.VMEM((NZ, 8, 128), F32),
            dma((11,)),
            dma((2,)), dma((2,)), dma((2,)), dma((2,)),
            dma((2,)), dma((2,)), dma((2,)), dma((2,)),
            dma(()), dma((16, 2)), dma(()), dma((16, 2)),
            dma(()), dma((16,)),
            dma((16,)), dma(()),
            dma((4,)), dma((4,)),
        ],
        compiler_params=pltpu.CompilerParams(
            collective_id=0, has_side_effects=True, vmem_limit_bytes=56 * 1024 * 1024
        ),
    )(dwa_coefs, layer_outs, avg_grads, attn_mixed)


def solution(mesh):
    in_specs = (P(None, "dp", "tensor"), P(None, "dp", "tensor"), P("dp", "tensor"), P())
    out_specs = (P(), P("dp", "tensor"))
    return jax.shard_map(local, mesh=mesh, in_specs=in_specs, out_specs=out_specs, check_vma=False)
```

```python
import jax
import jax.numpy as jnp
from jax import lax
from jax.experimental import pallas as pl
from jax.experimental.pallas import tpu as pltpu
from jax.sharding import PartitionSpec as P

MESH = pl.DeviceIdType.MESH
F32, BF16 = jnp.float32, jnp.bfloat16
NX, NY, NZ = 4, 4, 8
PAIRS_Z = [(1, 1), (0, 2), (0, 3), (1, 3)]
PAIRS_Y = [(0, 0), (0, 1), (1, 0), (1, 2), (2, 0), (2, 1), (2, 2), (2, 3), (3, 0), (3, 1), (3, 2), (3, 3)]
PAIRS = [(i, j) for i in range(4) for j in range(5) if j <= i + 1]


def kernel(
    co, lo_h, ag_h, at_h, coef_out, proj_out,
    lo, ag, ab, gt, outb, cb_c, cb_x, cb_y, cb_z,
    in_sem, gd_s, gd_r, gx_s, gx_r, gf_s, gf_r, ax_s, ax_r, f_r, c_s, c_r,
    *sums,
):
    dp, tk = lax.axis_index("dp"), lax.axis_index("tensor")
    z, y = dp // NY, dp % NY
    x, c = tk // 2, tk % 2
    xg = x + 1 - 2 * (x % 2)
    xa = NX - 1 - x

    def dev(x_, y_, z_, c_):
        return (z_ * NY + y_, x_ * 2 + c_)

    def send(src, dst, send_sem, recv_sem, where):
        copy = pltpu.make_async_remote_copy(
            src_ref=src, dst_ref=dst, send_sem=send_sem, recv_sem=recv_sem,
            device_id=where, device_id_type=MESH,
        )
        copy.start()

    def arrived(ref, sem):
        pltpu.make_async_copy(ref, ref, sem).wait()

    others_x = [(x + k) % NX for k in range(1, NX)]
    others_y = [(y + k) % NY for k in range(1, NY)]
    others_z = [(z + k) % NZ for k in range(1, NZ)]

    loads = {}

    def load(name, src, dst, i):
        loads[name] = pltpu.make_async_copy(src, dst, in_sem.at[i])
        loads[name].start()

    for part in range(2):
        rows = pl.ds(part * 512, 512)
        load(f"ag2{part}", ag_h.at[2, rows], ag.at[2, rows], part)
        load(f"ag3{part}", ag_h.at[3, rows], ag.at[3, rows], 11 + part)
    load("ab0", at_h.at[:, pl.ds(0, 256)], ab.at[0], 2)
    load("ab1", at_h.at[:, pl.ds(256, 256)], ab.at[1], 3)
    load("ag0", ag_h.at[0], ag.at[0], 4)
    load("ag1", ag_h.at[1], ag.at[1], 5)
    for j in range(5):
        load(f"lo{j}", lo_h.at[j], lo.at[j], 6 + j)

    barrier = pltpu.get_barrier_semaphore()
    greeted = [dev(x, y, z, 1 - c)]
    greeted += [dev(x_, y, z, c) for x_ in others_x]
    greeted += [dev(x, y_, z, c) for y_ in others_y]
    greeted += [dev(x, y, z_, c) for z_ in others_z]
    greeted += [dev(xa, y, z_, c) for z_ in others_z]
    for where in greeted:
        pl.semaphore_signal(barrier, inc=1, device_id=where, device_id_type=MESH)

    c2, c3 = co[2, 3], co[3, 3]

    def out_grad(i, _):
        rows = pl.ds(pl.multiple_of(i * 256, 256), 256)
        for yy in range(NY):
            cols = pl.ds(yy * 128, 128)
            first = c2 * ag[2, rows, cols].astype(F32)
            second = c3 * ag[3, rows, cols].astype(F32)
            turned = (first + second).astype(BF16).T
            for hh in range(2):
                gt[hh, yy, c, :, rows] = turned[hh * 64 : hh * 64 + 64]
        return 0

    for part in range(2):
        loads[f"ag2{part}"].wait()
        loads[f"ag3{part}"].wait()
        lax.fori_loop(2 * part, 2 * part + 2, out_grad, 0)
    pl.semaphore_wait(barrier, len(greeted))
    for j in range(2):
        send(gt.at[j, :, c], gt.at[j, :, c], gd_s.at[j], gd_r.at[j], dev(x, y, z, 1 - c))
        send(gt.at[j, :, c], gt.at[2 + j, :, c], gx_s.at[j], gx_r.at[j], dev(xg, y, z, c))
        loads[f"ab{j}"].wait()
        send(ab.at[j], ab.at[2 + j], ax_s.at[j], ax_r.at[j], dev(xa, y, z, c))

    up, down = dev(x, (y + 1) % NY, z, c), dev(x, (y + 3) % NY, z, c)

    class Sums:
        def __init__(self, refs):
            (
                self.pf, self.s1, self.r1, self.s2, self.r2, self.zs, self.za, self.zt, self.zb,
                self.out, self.y1_s, self.y1_r, self.y2_s, self.y2_r, self.z1_s, self.za_r,
                self.z2_s, self.zb_r, self.f_s,
            ) = refs

        def y_first(self, b):
            far = self.pf[b, (y + 2) % NY].astype(BF16)
            for i, where in enumerate((up, down)):
                self.s1[b, i] = far[4 * i : 4 * i + 4]
                send(self.s1.at[b, i], self.r1.at[b, i], self.y1_s, self.y1_r.at[b, i], where)

        def y_second(self, b):
            for i, (where, yc) in enumerate(((up, (y + 1) % NY), (down, (y + 3) % NY))):
                arrived(self.r1.at[b, i], self.y1_r.at[b, i])
                both, alone = pl.ds(4 * i, 4), pl.ds(4 - 4 * i, 4)
                self.s2[b, i, both] = (self.pf[b, yc, both] + self.r1[b, i].astype(F32)).astype(BF16)
                self.s2[b, i, alone] = self.pf[b, yc, alone].astype(BF16)
                send(self.s2.at[b, i], self.r2.at[b, i], self.y2_s, self.y2_r.at[b, i], where)

        def z_first(self, b, base):
            arrived(self.r2.at[b, 0], self.y2_r.at[b, 0])
            arrived(self.r2.at[b, 1], self.y2_r.at[b, 1])
            total = self.pf[b, y] + self.r2[b, 0].astype(F32) + self.r2[b, 1].astype(F32)
            self.pf[b, y] = total
            self.zs[b] = total.astype(BF16)
            far = 2 if b % 2 == 0 else 6
            for k, via, buf, n, sem in (
                (4, far, self.za, 2, self.za_r),
                (3, 1, self.za, 0, self.za_r),
                (5, 7, self.za, 1, self.za_r),
                (1, 1, self.zb, 0, self.zb_r),
                (7, 7, self.zb, 1, self.zb_r),
            ):
                src = self.zs.at[b, slot_of(k, base)]
                send(src, buf.at[b, n], self.z1_s, sem.at[b], dev(x, y, (z + via) % NZ, c))

        def z_second(self, b, base):
            arrived(self.za.at[b], self.za_r.at[b])
            for n, k in enumerate((2, 6)):
                part = self.pf[b, y, slot_of(k, base)] + self.za[b, n].astype(F32)
                if b % 2 == n:
                    part = part + self.za[b, 2].astype(F32)
                self.zt[b, n] = part.astype(BF16)
                there = dev(x, y, (z + k) % NZ, c)
                send(self.zt.at[b, n], self.zb.at[b, 2 + n], self.z2_s, self.zb_r.at[b], there)

        def home(self, b, base, own_plane, place):
            arrived(self.zb.at[b], self.zb_r.at[b])
            slot = slot_of(0, base)
            total = self.pf[b, y, slot]
            for k in range(4):
                total = total + self.zb[b, k].astype(F32)
            deliver(total, slot, self.out.at[b], self.f_s.at[b], base, own_plane, place)

        def ends(self, plan):
            arrived(self.s1, self.y1_s)
            arrived(self.s2, self.y2_s)
            arrived(self.zs.at[:, pl.ds(0, 5)], self.z1_s)
            arrived(self.zt, self.z2_s)
            delivered(self.out, self.f_s, plan)

    class SumsZ:
        def __init__(self, refs):
            (
                self.pf, self.zs, self.za, self.zt, self.zb, self.ys, self.yb, self.out,
                self.z1_s, self.za_r, self.z2_s, self.zb_r, self.y_s, self.yb_r, self.f_s,
            ) = refs

        def z_first(self, b, base):
            self.zs[b] = self.pf[b].astype(BF16)
            far = 2 if b % 2 == 0 else 6
            for k, via, buf, n, sem in (
                (4, far, self.za, 2, self.za_r),
                (3, 1, self.za, 0, self.za_r),
                (5, 7, self.za, 1, self.za_r),
                (1, 1, self.zb, 0, self.zb_r),
                (7, 7, self.zb, 1, self.zb_r),
            ):
                src = self.zs.at[b, slot_of(k, base)]
                send(src, buf.at[b, n], self.z1_s, sem.at[b], dev(x, y, (z + via) % NZ, c))

        def z_second(self, b, base):
            arrived(self.za.at[b], self.za_r.at[b])
            for n, k in enumerate((2, 6)):
                part = self.pf[b, slot_of(k, base)] + self.za[b, n].astype(F32)
                if b % 2 == n:
                    part = part + self.za[b, 2].astype(F32)
                self.zt[b, n] = part.astype(BF16)
                there = dev(x, y, (z + k) % NZ, c)
                send(self.zt.at[b, n], self.zb.at[b, 2 + n], self.z2_s, self.zb_r.at[b], there)

        def y_share(self, b, base):
            arrived(self.zb.at[b], self.zb_r.at[b])
            slot = slot_of(0, base)
            total = self.pf[b, slot]
            for k in range(4):
                total = total + self.zb[b, k].astype(F32)
            self.pf[b, slot] = total
            self.ys[b] = total.astype(BF16)
            for k in range(1, NY):
                yc = (y + k) % NY
                send(self.ys.at[b, yc], self.yb.at[b, k - 1], self.y_s, self.yb_r.at[b], dev(x, yc, z, c))

        def home(self, b, base, own_plane, place):
            arrived(self.yb.at[b], self.yb_r.at[b])
            slot = slot_of(0, base)
            total = self.pf[b, slot, y]
            for k in range(3):
                total = total + self.yb[b, k].astype(F32)
            deliver(total, slot, self.out.at[b], self.f_s.at[b], base, own_plane, place)

        def ends(self, plan):
            arrived(self.zs.at[:, pl.ds(0, 5)], self.z1_s)
            arrived(self.zt, self.z2_s)
            arrived(self.yb, self.y_s)
            delivered(self.out, self.f_s, plan)

    def deliver(total, slot, out, sem, base, own_plane, place):
        zh_ = 2 * base + slot // 4
        dst = outb.at[place(slot % 4)]

        def put(ref):
            for n in range(2):
                ref[n] = total[:, 128 * n : 128 * n + 128]

        if own_plane:

            @pl.when(zh_ == z)
            def _():
                put(dst)

            @pl.when(zh_ != z)
            def _():
                put(out)
                send(out, dst, sem, f_r, dev(x, y, zh_, c))

        else:
            put(out)
            send(out, dst, sem, f_r, dev(xa, y, zh_, c))

    def delivered(out, sems, plan):
        for b, (base, own_plane, _) in enumerate(plan):
            if own_plane:

                @pl.when(2 * base + slot_of(0, base) // 4 != z)
                def _():
                    arrived(out.at[b], sems.at[b])

            else:
                arrived(out.at[b], sems.at[b])

    def slot_of(k, base):
        return (z + k - 2 * base + 3 + NZ) % NZ

    ysum, zsum = Sums(sums[:19]), SumsZ(sums[19:])

    def product(g, a, b):
        term = jnp.dot(gt[g].reshape(512, 1024), ab[a], preferred_element_type=F32)
        ysum.pf[b] = term.reshape(NY, 8, 16, 256)
        ysum.y_first(b)

    def product_z(g, a, b):
        term = jnp.dot(gt[g].reshape(512, 1024), ab[a], preferred_element_type=F32)
        term = term.reshape(NY, 8, 16, 256)
        for yc in range(NY):
            zsum.pf[b, :, yc] = term[yc]
        zsum.z_first(b, plan_z[b][0])

    def loop(count, fn):
        def step(t, _):
            fn(t)
            return 0

        lax.fori_loop(0, count, step, 0)

    def plan_of(pairs):
        def place(g, a):
            return lambda u: (g % 2 * 4 + u, pl.ds(a % 2 * 2, 2))

        return [(x if g < 2 else xg, a < 2, place(g, a)) for g, a in pairs]

    plan_y, plan_z = plan_of(PAIRS_Y), plan_of(PAIRS_Z)

    def zf(*batches):
        for b in batches:
            ysum.z_first(b, plan_y[b][0])

    def zs(*batches):
        for b in batches:
            ysum.z_second(b, plan_y[b][0])

    def zh(*batches):
        for b in batches:
            ysum.home(b, *plan_y[b])

    def y2(*batches):
        for b in batches:
            ysum.y_second(b)

    def zz(b):
        zsum.z_second(b, plan_z[b][0])

    def zy(b):
        zsum.y_share(b, plan_z[b][0])

    def zn(b):
        zsum.home(b, *plan_z[b])

    def pass_on(j):
        src = gt.at[2 + j, :, c]
        arrived(src, gx_r.at[j])
        send(src, src, gf_s.at[j], gf_r.at[j], dev(x, y, z, 1 - c))

    def passed_on(j):
        arrived(gt.at[2 + j, :, 1 - c], gf_r.at[j])

    def coef_step(r, accs):
        rows = pl.ds(pl.multiple_of(r * 16, 16), 16)
        accs = list(accs)
        for q in range(4):
            cols = pl.ds(q * 128, 128)
            outs = [lo[j, rows, cols].astype(F32) for j in range(5)]
            grads = [ag[i, rows, cols].astype(F32) for i in range(4)]
            for n, (i, j) in enumerate(PAIRS):
                p = grads[i] * outs[j]
                accs[n] = accs[n] + (p[:8] + p[8:])
        return tuple(accs)

    def spread(buf, own, k0, targets, stage, size):
        for k, where in enumerate(targets):
            send(buf.at[own], buf.at[own], c_s.at[stage], c_r.at[stage], where)

    def settle(buf, own, stage, size):
        arrived(buf.at[pl.ds(0, size - 1)], c_r.at[stage])
        total = buf[0]
        for k in range(1, size):
            total = total + buf[k]
        return total

    def coef_local():
        for name in ["ag0", "ag1"] + [f"lo{j}" for j in range(5)]:
            loads[name].wait()
        zero = jnp.zeros((8, 128), F32)
        accs = lax.fori_loop(0, 64, coef_step, (zero,) * len(PAIRS))
        row = lax.broadcasted_iota(jnp.int32, (8, 128), 0)
        col = lax.broadcasted_iota(jnp.int32, (8, 128), 1)
        tile = zero
        for n, (i, j) in enumerate(PAIRS):
            total = jnp.sum(jnp.sum(accs[n], axis=0, keepdims=True), axis=1, keepdims=True)
            tile = jnp.where((row == i) & (col == j), jnp.broadcast_to(total, (8, 128)), tile)
        cb_c[c] = tile
        spread(cb_c, c, 0, [dev(x, y, z, 1 - c)], 0, 2)

    def coef_x():
        cb_x[x] = settle(cb_c, c, 0, 2)
        spread(cb_x, x, 0, [dev(x_, y, z, c) for x_ in others_x], 1, NX)

    def coef_y():
        cb_y[y] = settle(cb_x, x, 1, NX)
        spread(cb_y, y, 0, [dev(x, y_, z, c) for y_ in others_y], 2, NY)

    def coef_z():
        cb_z[z] = settle(cb_y, y, 2, NY)
        spread(cb_z, z, 0, [dev(x, y, z_, c) for z_ in others_z], 3, NZ)

    for j in range(2):
        arrived(gt.at[j, :, 1 - c], gd_r.at[j])
    product_z(1, 1, 0)
    loop(3, lambda t: product(t // 2, t % 2, t))
    y2(0, 1, 2)
    coef_local()
    zz(0)
    zf(0)

    arrived(ab.at[2], ax_r.at[0])
    pass_on(0)
    product_z(0, 2, 1)
    product(1, 2, 3)
    passed_on(0)
    loop(3, lambda t: product(2, t, 4 + t))
    zf(1, 2)
    y2(3)
    zs(0)
    y2(4)
    coef_x()
    y2(5, 6)
    zy(0)
    zs(1, 2)
    zz(1)
    zf(3)

    arrived(ab.at[3], ax_r.at[1])
    pass_on(1)
    product(2, 3, 7)
    product_z(0, 3, 2)
    product_z(1, 3, 3)
    passed_on(1)
    loop(4, lambda t: product(3, t, 8 + t))
    coef_y()
    zf(4, 5, 6)
    y2(7, 8, 9, 10, 11)
    zh(0, 1, 2)
    zn(0)
    zs(3, 4, 5, 6)
    zz(2)
    zf(7)
    coef_z()
    zz(3)
    zf(8)
    zh(3, 4)
    zf(9)
    zs(7)
    zh(5, 6)
    zf(10)
    zs(8)
    zy(1)
    zf(11)
    zs(9)
    zy(2)
    zh(7)
    zy(3)
    zs(10)
    zh(8)
    zs(11)
    zh(9)
    zn(1)
    zn(2)
    coef_out[...] = settle(cb_z, z, 3, NZ)
    zh(10)
    zn(3)
    zh(11)

    at_home = z // 4 == x // 2

    @pl.when(at_home)
    def _():
        arrived(outb.at[pl.ds(0, 6)], f_r)

    @pl.when(jnp.logical_not(at_home))
    def _():
        arrived(outb, f_r)

    proj_out[...] = outb[...]

    ysum.ends(plan_y)
    zsum.ends(plan_z)
    arrived(cb_c.at[0], c_s.at[0])
    arrived(cb_x.at[pl.ds(0, NX - 1)], c_s.at[1])
    arrived(cb_y.at[pl.ds(0, NY - 1)], c_s.at[2])
    arrived(cb_z.at[pl.ds(0, NZ - 1)], c_s.at[3])
    for j in range(2):
        arrived(ab.at[j], ax_s.at[j])
        arrived(gt.at[j, :, c], gx_s.at[j])
        arrived(gt.at[j, :, c], gd_s.at[j])
        arrived(gt.at[2 + j, :, c], gf_s.at[j])


OUT_COEF, OUT_PROJ = pltpu.VMEM((8, 128), F32), pltpu.VMEM((8, 4, 16, 128), F32)


def sums_scratch(count, width):
    dma = pltpu.SemaphoreType.DMA
    return [
        pltpu.VMEM((count, NY, 8, 16, width), F32),
        pltpu.VMEM((count, 2, 4, 16, width), BF16),
        pltpu.VMEM((count, 2, 4, 16, width), BF16),
        pltpu.VMEM((count, 2, 8, 16, width), BF16),
        pltpu.VMEM((count, 2, 8, 16, width), BF16),
        pltpu.VMEM((count, 8, 16, width), BF16),
        pltpu.VMEM((count, 3, 16, width), BF16),
        pltpu.VMEM((count, 2, 16, width), BF16),
        pltpu.VMEM((count, 4, 16, width), BF16),
        pltpu.VMEM((count, width // 128, 16, 128), F32),
        dma(()), dma((count, 2)), dma(()), dma((count, 2)),
        dma(()), dma((count,)), dma(()), dma((count,)),
        dma((count,)),
    ]


def sums_z_scratch(count):
    dma = pltpu.SemaphoreType.DMA
    return [
        pltpu.VMEM((count, 8, NY, 16, 256), F32),
        pltpu.VMEM((count, 8, NY, 16, 256), BF16),
        pltpu.VMEM((count, 3, NY, 16, 256), BF16),
        pltpu.VMEM((count, 2, NY, 16, 256), BF16),
        pltpu.VMEM((count, 4, NY, 16, 256), BF16),
        pltpu.VMEM((count, NY, 16, 256), BF16),
        pltpu.VMEM((count, 3, 16, 256), BF16),
        pltpu.VMEM((count, 2, 16, 128), F32),
        dma(()), dma((count,)), dma(()), dma((count,)),
        dma(()), dma((count,)), dma((count,)),
    ]


def local(layer_outs, avg_grads, attn_mixed, dwa_coefs):
    dma = pltpu.SemaphoreType.DMA
    anywhere = pl.BlockSpec(memory_space=pl.ANY)
    vmem = pl.BlockSpec(memory_space=pltpu.VMEM)
    coef, proj = pl.pallas_call(
        kernel,
        out_shape=(OUT_COEF, OUT_PROJ),
        in_specs=[pl.BlockSpec(memory_space=pltpu.SMEM), anywhere, anywhere, anywhere],
        out_specs=(vmem, vmem),
        scratch_shapes=[
            pltpu.VMEM((5, 1024, 512), BF16),
            pltpu.VMEM((4, 1024, 512), BF16),
            pltpu.VMEM((4, 1024, 256), BF16),
            pltpu.VMEM((4, NY, 2, 64, 1024), BF16),
            pltpu.VMEM((8, 4, 16, 128), F32),
            pltpu.VMEM((2, 8, 128), F32),
            pltpu.VMEM((NX, 8, 128), F32),
            pltpu.VMEM((NY, 8, 128), F32),
            pltpu.VMEM((NZ, 8, 128), F32),
            dma((13,)),
            dma((2,)), dma((2,)), dma((2,)), dma((2,)),
            dma((2,)), dma((2,)), dma((2,)), dma((2,)),
            dma(()), dma((4,)), dma((4,)),
            *sums_scratch(len(PAIRS_Y), 256),
            *sums_z_scratch(len(PAIRS_Z)),
        ],
        compiler_params=pltpu.CompilerParams(
            collective_id=0, has_side_effects=True, vmem_limit_bytes=56 * 1024 * 1024
        ),
    )(dwa_coefs, layer_outs, avg_grads, attn_mixed)
    coef = pltpu.with_memory_space_constraint(coef, pltpu.VMEM)
    proj = pltpu.with_memory_space_constraint(proj, pltpu.VMEM)
    return pl.pallas_call(
        lay_out,
        out_shape=(jax.ShapeDtypeStruct((4, 5), F32), jax.ShapeDtypeStruct((128, 512), F32)),
        in_specs=[vmem, vmem],
        out_specs=(vmem, vmem),
    )(coef, proj)


def lay_out(coef, proj, coef_out, proj_out):
    coef_out[...] = coef[:4, :5]
    for block in range(8):
        for j in range(4):
            proj_out[pl.ds(block * 16, 16), pl.ds(j * 128, 128)] = proj[block, j]


def solution(mesh):
    in_specs = (P(None, "dp", "tensor"), P(None, "dp", "tensor"), P("dp", "tensor"), P())
    out_specs = (P(), P("dp", "tensor"))
    return jax.shard_map(local, mesh=mesh, in_specs=in_specs, out_specs=out_specs, check_vma=False)
```

```python
import jax
import jax.numpy as jnp
from jax import lax
from jax.experimental import pallas as pl
from jax.experimental.pallas import tpu as pltpu
from jax.sharding import PartitionSpec as P

MESH = pl.DeviceIdType.MESH
F32, BF16 = jnp.float32, jnp.bfloat16
NX, NY, NZ = 4, 4, 8
PAIRS_Z = [(1, 1), (0, 2), (1, 2), (3, 3)]
PAIRS_Y = [(0, 0), (0, 1), (1, 0), (2, 0), (2, 1), (2, 2), (3, 2), (3, 1), (3, 0)]
HALVES = [(g, t) for t in range(2) for g in range(3)]
PAIRS = [(i, j) for i in range(4) for j in range(5) if j <= i + 1]


def kernel(
    co, lo_h, ag_h, at_h, coef_out, proj_out,
    lo, ag, ab, gt, outb, cb_c, cb_x, cb_y, cb_z,
    in_sem, gd_s, gd_r, gx_s, gx_r, gf_s, gf_r, ax_s, ax_r, f_r, c_s, c_r,
    *sums,
):
    dp, tk = lax.axis_index("dp"), lax.axis_index("tensor")
    z, y = dp // NY, dp % NY
    x, c = tk // 2, tk % 2
    xg = x + 1 - 2 * (x % 2)
    xa = NX - 1 - x

    def dev(x_, y_, z_, c_):
        return (z_ * NY + y_, x_ * 2 + c_)

    def send(src, dst, send_sem, recv_sem, where):
        copy = pltpu.make_async_remote_copy(
            src_ref=src, dst_ref=dst, send_sem=send_sem, recv_sem=recv_sem,
            device_id=where, device_id_type=MESH,
        )
        copy.start()

    def arrived(ref, sem):
        pltpu.make_async_copy(ref, ref, sem).wait()

    others_x = [(x + k) % NX for k in range(1, NX)]
    others_y = [(y + k) % NY for k in range(1, NY)]
    others_z = [(z + k) % NZ for k in range(1, NZ)]

    loads = {}

    def load(name, src, dst, i):
        loads[name] = pltpu.make_async_copy(src, dst, in_sem.at[i])
        loads[name].start()

    for part in range(2):
        rows = pl.ds(part * 512, 512)
        load(f"ag2{part}", ag_h.at[2, rows], ag.at[2, rows], part)
        load(f"ag3{part}", ag_h.at[3, rows], ag.at[3, rows], 11 + part)
    load("ab0", at_h.at[:, pl.ds(0, 256)], ab.at[0], 2)
    load("ab1", at_h.at[:, pl.ds(256, 256)], ab.at[1], 3)
    load("ag0", ag_h.at[0], ag.at[0], 4)
    load("ag1", ag_h.at[1], ag.at[1], 5)
    for j in range(5):
        load(f"lo{j}", lo_h.at[j], lo.at[j], 6 + j)

    barrier = pltpu.get_barrier_semaphore()
    greeted = [dev(x, y, z, 1 - c)]
    greeted += [dev(x_, y, z, c) for x_ in others_x]
    greeted += [dev(x, y_, z, c) for y_ in others_y]
    greeted += [dev(x, y, z_, c) for z_ in others_z]
    greeted += [dev(xa, y, z_, c) for z_ in others_z]
    for where in greeted:
        pl.semaphore_signal(barrier, inc=1, device_id=where, device_id_type=MESH)

    def ab_piece(n, j):
        return ab.at[n] if j == 0 else ab.at[n + 1, :, pl.ds(128 * (j - 1), 128)]

    c2, c3 = co[2, 3], co[3, 3]

    def out_grad(i, _):
        rows = pl.ds(pl.multiple_of(i * 256, 256), 256)
        for yy in range(NY):
            cols = pl.ds(yy * 128, 128)
            first = c2 * ag[2, rows, cols].astype(F32)
            second = c3 * ag[3, rows, cols].astype(F32)
            turned = (first + second).astype(BF16).T
            for hh in range(2):
                gt[hh, yy, c, :, rows] = turned[hh * 64 : hh * 64 + 64]
        return 0

    for part in range(2):
        loads[f"ag2{part}"].wait()
        loads[f"ag3{part}"].wait()
        lax.fori_loop(2 * part, 2 * part + 2, out_grad, 0)
    pl.semaphore_wait(barrier, len(greeted))
    for j in range(2):
        send(gt.at[j, :, c], gt.at[j, :, c], gd_s.at[j], gd_r.at[j], dev(x, y, z, 1 - c))
        send(gt.at[j, :, c], gt.at[2 + j, :, c], gx_s.at[j], gx_r.at[j], dev(xg, y, z, c))
        loads[f"ab{j}"].wait()
        for n in ((0,), (1, 2))[j]:
            send(ab_piece(0, n), ab_piece(2, n), ax_s.at[n], ax_r.at[n], dev(xa, y, z, c))

    up, down = dev(x, (y + 1) % NY, z, c), dev(x, (y + 3) % NY, z, c)

    class Sums:
        def __init__(self, refs):
            (
                self.pf, self.s1, self.r1, self.s2, self.r2, self.zs, self.za, self.zt, self.zb,
                self.out, self.y1_s, self.y1_r, self.y2_s, self.y2_r, self.z1_s, self.za_r,
                self.z2_s, self.zb_r, self.f_s,
            ) = refs

        def y_first(self, b):
            far = self.pf[b, (y + 2) % NY].astype(BF16)
            for i, where in enumerate((up, down)):
                self.s1[b, i] = far[4 * i : 4 * i + 4]
                send(self.s1.at[b, i], self.r1.at[b, i], self.y1_s, self.y1_r.at[b, i], where)

        def y_second(self, b):
            for i, (where, yc) in enumerate(((up, (y + 1) % NY), (down, (y + 3) % NY))):
                arrived(self.r1.at[b, i], self.y1_r.at[b, i])
                both, alone = pl.ds(4 * i, 4), pl.ds(4 - 4 * i, 4)
                self.s2[b, i, both] = (self.pf[b, yc, both] + self.r1[b, i].astype(F32)).astype(BF16)
                self.s2[b, i, alone] = self.pf[b, yc, alone].astype(BF16)
                send(self.s2.at[b, i], self.r2.at[b, i], self.y2_s, self.y2_r.at[b, i], where)

        def z_first(self, b, base):
            arrived(self.r2.at[b, 0], self.y2_r.at[b, 0])
            arrived(self.r2.at[b, 1], self.y2_r.at[b, 1])
            total = self.pf[b, y] + self.r2[b, 0].astype(F32) + self.r2[b, 1].astype(F32)
            self.pf[b, y] = total
            self.zs[b] = total.astype(BF16)
            far = 2 if b % 2 == 0 else 6
            for k, via, buf, n, sem in (
                (4, far, self.za, 2, self.za_r),
                (3, 1, self.za, 0, self.za_r),
                (5, 7, self.za, 1, self.za_r),
                (1, 1, self.zb, 0, self.zb_r),
                (7, 7, self.zb, 1, self.zb_r),
            ):
                src = self.zs.at[b, slot_of(k, base)]
                send(src, buf.at[b, n], self.z1_s, sem.at[b], dev(x, y, (z + via) % NZ, c))

        def z_second(self, b, base):
            arrived(self.za.at[b], self.za_r.at[b])
            for n, k in enumerate((2, 6)):
                part = self.pf[b, y, slot_of(k, base)] + self.za[b, n].astype(F32)
                if b % 2 == n:
                    part = part + self.za[b, 2].astype(F32)
                self.zt[b, n] = part.astype(BF16)
                there = dev(x, y, (z + k) % NZ, c)
                send(self.zt.at[b, n], self.zb.at[b, 2 + n], self.z2_s, self.zb_r.at[b], there)

        def home(self, b, base, own_plane, place):
            arrived(self.zb.at[b], self.zb_r.at[b])
            slot = slot_of(0, base)
            total = self.pf[b, y, slot]
            for k in range(4):
                total = total + self.zb[b, k].astype(F32)
            deliver(total, slot, self.out.at[b], self.f_s.at[b], base, own_plane, place)

        def ends(self, plan):
            arrived(self.s1, self.y1_s)
            arrived(self.s2, self.y2_s)
            arrived(self.zs.at[:, pl.ds(0, 5)], self.z1_s)
            arrived(self.zt, self.z2_s)
            delivered(self.out, self.f_s, plan)

    class SumsZ:
        def __init__(self, refs):
            (
                self.pf, self.zs, self.za, self.zt, self.zb, self.ys, self.yb, self.out,
                self.z1_s, self.za_r, self.z2_s, self.zb_r, self.y_s, self.yb_r, self.f_s,
            ) = refs

        def z_first(self, b, base):
            self.zs[b] = self.pf[b].astype(BF16)
            far = 2 if b % 2 == 0 else 6
            for k, via, buf, n, sem in (
                (4, far, self.za, 2, self.za_r),
                (3, 1, self.za, 0, self.za_r),
                (5, 7, self.za, 1, self.za_r),
                (1, 1, self.zb, 0, self.zb_r),
                (7, 7, self.zb, 1, self.zb_r),
            ):
                src = self.zs.at[b, slot_of(k, base)]
                send(src, buf.at[b, n], self.z1_s, sem.at[b], dev(x, y, (z + via) % NZ, c))

        def z_second(self, b, base):
            arrived(self.za.at[b], self.za_r.at[b])
            for n, k in enumerate((2, 6)):
                part = self.pf[b, slot_of(k, base)] + self.za[b, n].astype(F32)
                if b % 2 == n:
                    part = part + self.za[b, 2].astype(F32)
                self.zt[b, n] = part.astype(BF16)
                there = dev(x, y, (z + k) % NZ, c)
                send(self.zt.at[b, n], self.zb.at[b, 2 + n], self.z2_s, self.zb_r.at[b], there)

        def y_share(self, b, base):
            arrived(self.zb.at[b], self.zb_r.at[b])
            slot = slot_of(0, base)
            total = self.pf[b, slot]
            for k in range(4):
                total = total + self.zb[b, k].astype(F32)
            self.pf[b, slot] = total
            self.ys[b] = total.astype(BF16)
            for k in range(1, NY):
                yc = (y + k) % NY
                send(self.ys.at[b, yc], self.yb.at[b, k - 1], self.y_s, self.yb_r.at[b], dev(x, yc, z, c))

        def home(self, b, base, own_plane, place):
            arrived(self.yb.at[b], self.yb_r.at[b])
            slot = slot_of(0, base)
            total = self.pf[b, slot, y]
            for k in range(3):
                total = total + self.yb[b, k].astype(F32)
            deliver(total, slot, self.out.at[b], self.f_s.at[b], base, own_plane, place)

        def ends(self, plan):
            arrived(self.zs.at[:, pl.ds(0, 5)], self.z1_s)
            arrived(self.zt, self.z2_s)
            arrived(self.yb, self.y_s)
            delivered(self.out, self.f_s, plan)

    def deliver(total, slot, out, sem, base, own_plane, place):
        zh_ = 2 * base + slot // 4
        dst = outb.at[place(slot % 4)]

        def put(ref):
            for n in range(total.shape[1] // 128):
                ref[n] = total[:, 128 * n : 128 * n + 128].astype(BF16)

        if own_plane:

            @pl.when(zh_ == z)
            def _():
                put(dst)

            @pl.when(zh_ != z)
            def _():
                put(out)
                send(out, dst, sem, f_r, dev(x, y, zh_, c))

        else:
            put(out)
            send(out, dst, sem, f_r, dev(xa, y, zh_, c))

    def delivered(out, sems, plan):
        for b, (base, own_plane, _) in enumerate(plan):
            if own_plane:

                @pl.when(2 * base + slot_of(0, base) // 4 != z)
                def _():
                    arrived(out.at[b], sems.at[b])

            else:
                arrived(out.at[b], sems.at[b])

    def slot_of(k, base):
        return (z + k - 2 * base + 3 + NZ) % NZ

    ysum, half, zsum = Sums(sums[:19]), Sums(sums[19:38]), SumsZ(sums[38:])

    def product(g, a, b):
        term = jnp.dot(gt[g].reshape(512, 1024), ab[a], preferred_element_type=F32)
        ysum.pf[b] = term.reshape(NY, 8, 16, 256)
        ysum.y_first(b)

    def product_half(g, t, b):
        right = ab[3, :, t * 128 : t * 128 + 128]
        term = jnp.dot(gt[g].reshape(512, 1024), right, preferred_element_type=F32)
        half.pf[b] = term.reshape(NY, 8, 16, 128)
        half.y_first(b)

    def product_z(g, a, b):
        term = jnp.dot(gt[g].reshape(512, 1024), ab[a], preferred_element_type=F32)
        term = term.reshape(NY, 8, 16, 256)
        for yc in range(NY):
            zsum.pf[b, :, yc] = term[yc]
        zsum.z_first(b, plan_z[b][0])

    def loop(count, fn):
        def step(t, _):
            fn(t)
            return 0

        lax.fori_loop(0, count, step, 0)

    def plan_of(pairs):
        def place(g, a):
            return lambda u: (g % 2 * 4 + u, pl.ds(a % 2 * 2, 2))

        return [(x if g < 2 else xg, a < 2, place(g, a)) for g, a in pairs]

    def half_place(g, t):
        return lambda u: (g % 2 * 4 + u, pl.ds(2 + t, 1))

    plan_y, plan_z = plan_of(PAIRS_Y), plan_of(PAIRS_Z)
    plan_half = [(x if g < 2 else xg, False, half_place(g, t)) for g, t in HALVES]

    def zf(*batches):
        for b in batches:
            ysum.z_first(b, plan_y[b][0])

    def zs(*batches):
        for b in batches:
            ysum.z_second(b, plan_y[b][0])

    def zh(*batches):
        for b in batches:
            ysum.home(b, *plan_y[b])

    def y2(*batches):
        for b in batches:
            ysum.y_second(b)

    def hf(*batches):
        for b in batches:
            half.z_first(b, plan_half[b][0])

    def hs(*batches):
        for b in batches:
            half.z_second(b, plan_half[b][0])

    def hh(*batches):
        for b in batches:
            half.home(b, *plan_half[b])

    def h2(*batches):
        for b in batches:
            half.y_second(b)

    def zz(b):
        zsum.z_second(b, plan_z[b][0])

    def zy(b):
        zsum.y_share(b, plan_z[b][0])

    def zn(b):
        zsum.home(b, *plan_z[b])

    def pass_on(j):
        src = gt.at[2 + j, :, c]
        arrived(src, gx_r.at[j])
        send(src, src, gf_s.at[j], gf_r.at[j], dev(x, y, z, 1 - c))

    def passed_on(j):
        arrived(gt.at[2 + j, :, 1 - c], gf_r.at[j])

    def coef_step(r, accs):
        rows = pl.ds(pl.multiple_of(r * 16, 16), 16)
        accs = list(accs)
        for q in range(4):
            cols = pl.ds(q * 128, 128)
            outs = [lo[j, rows, cols].astype(F32) for j in range(5)]
            grads = [ag[i, rows, cols].astype(F32) for i in range(4)]
            for n, (i, j) in enumerate(PAIRS):
                p = grads[i] * outs[j]
                accs[n] = accs[n] + (p[:8] + p[8:])
        return tuple(accs)

    def spread(buf, own, k0, targets, stage, size):
        for k, where in enumerate(targets):
            send(buf.at[own], buf.at[own], c_s.at[stage], c_r.at[stage], where)

    def settle(buf, own, stage, size):
        arrived(buf.at[pl.ds(0, size - 1)], c_r.at[stage])
        total = buf[0]
        for k in range(1, size):
            total = total + buf[k]
        return total

    def coef_local():
        for name in ["ag0", "ag1"] + [f"lo{j}" for j in range(5)]:
            loads[name].wait()
        zero = jnp.zeros((8, 128), F32)
        accs = lax.fori_loop(0, 64, coef_step, (zero,) * len(PAIRS))
        row = lax.broadcasted_iota(jnp.int32, (8, 128), 0)
        col = lax.broadcasted_iota(jnp.int32, (8, 128), 1)
        tile = zero
        for n, (i, j) in enumerate(PAIRS):
            total = jnp.sum(jnp.sum(accs[n], axis=0, keepdims=True), axis=1, keepdims=True)
            tile = jnp.where((row == i) & (col == j), jnp.broadcast_to(total, (8, 128)), tile)
        cb_c[c] = tile
        spread(cb_c, c, 0, [dev(x, y, z, 1 - c)], 0, 2)

    def coef_x():
        cb_x[x] = settle(cb_c, c, 0, 2)
        spread(cb_x, x, 0, [dev(x_, y, z, c) for x_ in others_x], 1, NX)

    def coef_y():
        cb_y[y] = settle(cb_x, x, 1, NX)
        spread(cb_y, y, 0, [dev(x, y_, z, c) for y_ in others_y], 2, NY)

    def coef_z():
        cb_z[z] = settle(cb_y, y, 2, NY)
        spread(cb_z, z, 0, [dev(x, y, z_, c) for z_ in others_z], 3, NZ)

    for j in range(2):
        arrived(gt.at[j, :, 1 - c], gd_r.at[j])
    product_z(1, 1, 0)
    loop(3, lambda t: product(t // 2, t % 2, t))
    y2(0, 1, 2)
    coef_local()
    zz(0)
    zf(0)

    arrived(ab_piece(2, 0), ax_r.at[0])
    pass_on(0)
    product_z(0, 2, 1)
    product_z(1, 2, 2)
    passed_on(0)
    loop(3, lambda t: product(2, t, 3 + t))
    zf(1, 2)
    zs(0)

    arrived(ab_piece(2, 1), ax_r.at[1])
    loop(3, lambda t: product_half(t, 0, t))
    coef_x()
    y2(3, 4, 5)
    zy(0)
    zs(1, 2)
    zz(1)
    h2(0, 1, 2)
    zz(2)

    arrived(ab_piece(2, 2), ax_r.at[2])
    pass_on(1)
    loop(3, lambda t: product_half(t, 1, 3 + t))
    zf(3, 4)
    passed_on(1)
    product_z(3, 3, 3)
    loop(3, lambda t: product(3, 2 - t, 6 + t))
    coef_y()
    zf(5)
    h2(3, 4, 5)
    hf(0, 1)
    y2(6)
    hf(2)
    y2(7, 8)
    zs(3, 4, 5)
    zh(0, 1, 2)
    zn(0)
    zy(1)
    zy(2)
    hs(0, 1)
    hf(3)
    zz(3)
    hf(4, 5)
    hs(2)
    coef_z()
    zf(6)
    zh(3, 4, 5)
    zf(7)
    hs(3, 4)
    zf(8)
    hh(0, 1, 2)
    hs(5)
    zs(6)
    zy(3)
    zs(7)
    hh(3, 4, 5)
    zs(8)
    zn(1)
    zn(2)
    coef_out[...] = settle(cb_z, z, 3, NZ)
    zh(6, 7)
    zn(3)
    zh(8)

    at_home = z // 4 == x // 2

    @pl.when(at_home)
    def _():
        arrived(outb.at[pl.ds(0, 6)], f_r)

    @pl.when(jnp.logical_not(at_home))
    def _():
        arrived(outb, f_r)

    proj_out[...] = outb[...]

    ysum.ends(plan_y)
    half.ends(plan_half)
    zsum.ends(plan_z)
    arrived(cb_c.at[0], c_s.at[0])
    arrived(cb_x.at[pl.ds(0, NX - 1)], c_s.at[1])
    arrived(cb_y.at[pl.ds(0, NY - 1)], c_s.at[2])
    arrived(cb_z.at[pl.ds(0, NZ - 1)], c_s.at[3])
    for j in range(2):
        arrived(gt.at[j, :, c], gx_s.at[j])
        arrived(gt.at[j, :, c], gd_s.at[j])
        arrived(gt.at[2 + j, :, c], gf_s.at[j])
    for j in range(3):
        arrived(ab_piece(0, j), ax_s.at[j])


OUT_COEF, OUT_PROJ = pltpu.VMEM((8, 128), F32), pltpu.VMEM((8, 4, 16, 128), BF16)


def sums_scratch(count, width):
    dma = pltpu.SemaphoreType.DMA
    return [
        pltpu.VMEM((count, NY, 8, 16, width), F32),
        pltpu.VMEM((count, 2, 4, 16, width), BF16),
        pltpu.VMEM((count, 2, 4, 16, width), BF16),
        pltpu.VMEM((count, 2, 8, 16, width), BF16),
        pltpu.VMEM((count, 2, 8, 16, width), BF16),
        pltpu.VMEM((count, 8, 16, width), BF16),
        pltpu.VMEM((count, 3, 16, width), BF16),
        pltpu.VMEM((count, 2, 16, width), BF16),
        pltpu.VMEM((count, 4, 16, width), BF16),
        pltpu.VMEM((count, width // 128, 16, 128), BF16),
        dma(()), dma((count, 2)), dma(()), dma((count, 2)),
        dma(()), dma((count,)), dma(()), dma((count,)),
        dma((count,)),
    ]


def sums_z_scratch(count):
    dma = pltpu.SemaphoreType.DMA
    return [
        pltpu.VMEM((count, 8, NY, 16, 256), F32),
        pltpu.VMEM((count, 8, NY, 16, 256), BF16),
        pltpu.VMEM((count, 3, NY, 16, 256), BF16),
        pltpu.VMEM((count, 2, NY, 16, 256), BF16),
        pltpu.VMEM((count, 4, NY, 16, 256), BF16),
        pltpu.VMEM((count, NY, 16, 256), BF16),
        pltpu.VMEM((count, 3, 16, 256), BF16),
        pltpu.VMEM((count, 2, 16, 128), BF16),
        dma(()), dma((count,)), dma(()), dma((count,)),
        dma(()), dma((count,)), dma((count,)),
    ]


def local(layer_outs, avg_grads, attn_mixed, dwa_coefs):
    dma = pltpu.SemaphoreType.DMA
    anywhere = pl.BlockSpec(memory_space=pl.ANY)
    vmem = pl.BlockSpec(memory_space=pltpu.VMEM)
    coef, proj = pl.pallas_call(
        kernel,
        out_shape=(OUT_COEF, OUT_PROJ),
        in_specs=[pl.BlockSpec(memory_space=pltpu.SMEM), anywhere, anywhere, anywhere],
        out_specs=(vmem, vmem),
        scratch_shapes=[
            pltpu.VMEM((5, 1024, 512), BF16),
            pltpu.VMEM((4, 1024, 512), BF16),
            pltpu.VMEM((4, 1024, 256), BF16),
            pltpu.VMEM((4, NY, 2, 64, 1024), BF16),
            pltpu.VMEM((8, 4, 16, 128), BF16),
            pltpu.VMEM((2, 8, 128), F32),
            pltpu.VMEM((NX, 8, 128), F32),
            pltpu.VMEM((NY, 8, 128), F32),
            pltpu.VMEM((NZ, 8, 128), F32),
            dma((13,)),
            dma((2,)), dma((2,)), dma((2,)), dma((2,)),
            dma((2,)), dma((2,)), dma((3,)), dma((3,)),
            dma(()), dma((4,)), dma((4,)),
            *sums_scratch(len(PAIRS_Y), 256),
            *sums_scratch(len(HALVES), 128),
            *sums_z_scratch(len(PAIRS_Z)),
        ],
        compiler_params=pltpu.CompilerParams(
            collective_id=0, has_side_effects=True, vmem_limit_bytes=56 * 1024 * 1024
        ),
    )(dwa_coefs, layer_outs, avg_grads, attn_mixed)
    coef = pltpu.with_memory_space_constraint(coef, pltpu.VMEM)
    proj = pltpu.with_memory_space_constraint(proj, pltpu.VMEM)
    return pl.pallas_call(
        lay_out,
        out_shape=(jax.ShapeDtypeStruct((4, 5), F32), jax.ShapeDtypeStruct((128, 512), F32)),
        in_specs=[vmem, vmem],
        out_specs=(vmem, vmem),
    )(coef, proj)


def lay_out(coef, proj, coef_out, proj_out):
    coef_out[...] = coef[:4, :5]
    for block in range(8):
        for j in range(4):
            proj_out[pl.ds(block * 16, 16), pl.ds(j * 128, 128)] = proj[block, j].astype(F32)


def solution(mesh):
    in_specs = (P(None, "dp", "tensor"), P(None, "dp", "tensor"), P("dp", "tensor"), P())
    out_specs = (P(), P("dp", "tensor"))
    return jax.shard_map(local, mesh=mesh, in_specs=in_specs, out_specs=out_specs, check_vma=False)
```

```python
import jax
import jax.numpy as jnp
from jax import lax
from jax.experimental import pallas as pl
from jax.experimental.pallas import tpu as pltpu
from jax.sharding import PartitionSpec as P

MESH = pl.DeviceIdType.MESH
F32, BF16 = jnp.float32, jnp.bfloat16
NX, NY, NZ = 4, 4, 8
PAIRS_Z = [(1, 1), (0, 2), (1, 2), (2, 2), (3, 3)]
PAIRS_Y = [(0, 0), (0, 1), (1, 0), (2, 0), (2, 1), (3, 2), (3, 1), (3, 0)]
HALVES = [(g, t) for t in range(2) for g in range(3)]
PAIRS = [(i, j) for i in range(4) for j in range(5) if j <= i + 1]


def kernel(
    co, lo_h, ag_h, at_h, coef_out, proj_out,
    lo, ag, ab, gt, outb, cb_c, cb_x, cb_y, cb_z,
    in_sem, gd_s, gd_r, gx_s, gx_r, gf_s, gf_r, ax_s, ax_r, f_r, c_s, c_r,
    *sums,
):
    dp, tk = lax.axis_index("dp"), lax.axis_index("tensor")
    z, y = dp // NY, dp % NY
    x, c = tk // 2, tk % 2
    xg = x + 1 - 2 * (x % 2)
    xa = NX - 1 - x

    def dev(x_, y_, z_, c_):
        return (z_ * NY + y_, x_ * 2 + c_)

    def send(src, dst, send_sem, recv_sem, where):
        copy = pltpu.make_async_remote_copy(
            src_ref=src, dst_ref=dst, send_sem=send_sem, recv_sem=recv_sem,
            device_id=where, device_id_type=MESH,
        )
        copy.start()

    def arrived(ref, sem):
        pltpu.make_async_copy(ref, ref, sem).wait()

    others_x = [(x + k) % NX for k in range(1, NX)]
    others_y = [(y + k) % NY for k in range(1, NY)]
    others_z = [(z + k) % NZ for k in range(1, NZ)]

    loads = {}

    def load(name, src, dst, i):
        loads[name] = pltpu.make_async_copy(src, dst, in_sem.at[i])
        loads[name].start()

    for part in range(2):
        rows = pl.ds(part * 512, 512)
        load(f"ag2{part}", ag_h.at[2, rows], ag.at[2, rows], part)
        load(f"ag3{part}", ag_h.at[3, rows], ag.at[3, rows], 11 + part)
    load("ab0", at_h.at[:, pl.ds(0, 256)], ab.at[0], 2)
    load("ab1", at_h.at[:, pl.ds(256, 256)], ab.at[1], 3)
    load("ag0", ag_h.at[0], ag.at[0], 4)
    load("ag1", ag_h.at[1], ag.at[1], 5)
    for j in range(5):
        load(f"lo{j}", lo_h.at[j], lo.at[j], 6 + j)

    barrier = pltpu.get_barrier_semaphore()
    greeted = [dev(x, y, z, 1 - c)]
    greeted += [dev(x_, y, z, c) for x_ in others_x]
    greeted += [dev(x, y_, z, c) for y_ in others_y]
    greeted += [dev(x, y, z_, c) for z_ in others_z]
    greeted += [dev(xa, y, z_, c) for z_ in others_z]
    for where in greeted:
        pl.semaphore_signal(barrier, inc=1, device_id=where, device_id_type=MESH)

    def ab_piece(n, j):
        return ab.at[n] if j == 0 else ab.at[n + 1, :, pl.ds(128 * (j - 1), 128)]

    c2, c3 = co[2, 3], co[3, 3]

    def out_grad(i, _):
        rows = pl.ds(pl.multiple_of(i * 256, 256), 256)
        for yy in range(NY):
            cols = pl.ds(yy * 128, 128)
            first = c2 * ag[2, rows, cols].astype(F32)
            second = c3 * ag[3, rows, cols].astype(F32)
            turned = (first + second).astype(BF16).T
            for hh in range(2):
                gt[hh, yy, c, :, rows] = turned[hh * 64 : hh * 64 + 64]
        return 0

    for part in range(2):
        loads[f"ag2{part}"].wait()
        loads[f"ag3{part}"].wait()
        lax.fori_loop(2 * part, 2 * part + 2, out_grad, 0)
    pl.semaphore_wait(barrier, len(greeted))
    for j in range(2):
        send(gt.at[j, :, c], gt.at[j, :, c], gd_s.at[j], gd_r.at[j], dev(x, y, z, 1 - c))
        send(gt.at[j, :, c], gt.at[2 + j, :, c], gx_s.at[j], gx_r.at[j], dev(xg, y, z, c))
        loads[f"ab{j}"].wait()
        for n in ((0,), (1, 2))[j]:
            send(ab_piece(0, n), ab_piece(2, n), ax_s.at[n], ax_r.at[n], dev(xa, y, z, c))

    up, down = dev(x, (y + 1) % NY, z, c), dev(x, (y + 3) % NY, z, c)

    class Sums:
        def __init__(self, refs):
            (
                self.pf, self.s1, self.r1, self.s2, self.r2, self.zs, self.za, self.zt, self.zb,
                self.out, self.y1_s, self.y1_r, self.y2_s, self.y2_r, self.z1_s, self.za_r,
                self.z2_s, self.zb_r, self.f_s,
            ) = refs

        def y_first(self, b):
            far = self.pf[b, (y + 2) % NY].astype(BF16)
            for i, where in enumerate((up, down)):
                self.s1[b, i] = far[4 * i : 4 * i + 4]
                send(self.s1.at[b, i], self.r1.at[b, i], self.y1_s, self.y1_r.at[b, i], where)

        def y_second(self, b):
            for i, (where, yc) in enumerate(((up, (y + 1) % NY), (down, (y + 3) % NY))):
                arrived(self.r1.at[b, i], self.y1_r.at[b, i])
                both, alone = pl.ds(4 * i, 4), pl.ds(4 - 4 * i, 4)
                self.s2[b, i, both] = (self.pf[b, yc, both] + self.r1[b, i].astype(F32)).astype(BF16)
                self.s2[b, i, alone] = self.pf[b, yc, alone].astype(BF16)
                send(self.s2.at[b, i], self.r2.at[b, i], self.y2_s, self.y2_r.at[b, i], where)

        def z_first(self, b, base):
            arrived(self.r2.at[b, 0], self.y2_r.at[b, 0])
            arrived(self.r2.at[b, 1], self.y2_r.at[b, 1])
            total = self.pf[b, y] + self.r2[b, 0].astype(F32) + self.r2[b, 1].astype(F32)
            self.pf[b, y] = total
            self.zs[b] = total.astype(BF16)
            far = 2 if b % 2 == 0 else 6
            for k, via, buf, n, sem in (
                (4, far, self.za, 2, self.za_r),
                (3, 1, self.za, 0, self.za_r),
                (5, 7, self.za, 1, self.za_r),
                (1, 1, self.zb, 0, self.zb_r),
                (7, 7, self.zb, 1, self.zb_r),
            ):
                src = self.zs.at[b, slot_of(k, base)]
                send(src, buf.at[b, n], self.z1_s, sem.at[b], dev(x, y, (z + via) % NZ, c))

        def z_second(self, b, base):
            arrived(self.za.at[b], self.za_r.at[b])
            for n, k in enumerate((2, 6)):
                part = self.pf[b, y, slot_of(k, base)] + self.za[b, n].astype(F32)
                if b % 2 == n:
                    part = part + self.za[b, 2].astype(F32)
                self.zt[b, n] = part.astype(BF16)
                there = dev(x, y, (z + k) % NZ, c)
                send(self.zt.at[b, n], self.zb.at[b, 2 + n], self.z2_s, self.zb_r.at[b], there)

        def home(self, b, base, own_plane, place):
            arrived(self.zb.at[b], self.zb_r.at[b])
            slot = slot_of(0, base)
            total = self.pf[b, y, slot]
            for k in range(4):
                total = total + self.zb[b, k].astype(F32)
            deliver(total, slot, self.out.at[b], self.f_s.at[b], base, own_plane, place)

        def ends(self, plan):
            arrived(self.s1, self.y1_s)
            arrived(self.s2, self.y2_s)
            arrived(self.zs.at[:, pl.ds(0, 5)], self.z1_s)
            arrived(self.zt, self.z2_s)
            delivered(self.out, self.f_s, plan)

    class SumsZ:
        def __init__(self, refs):
            (
                self.pf, self.zs, self.za, self.zt, self.zb, self.ys, self.yb, self.out,
                self.z1_s, self.za_r, self.z2_s, self.zb_r, self.y_s, self.yb_r, self.f_s,
            ) = refs

        def z_first(self, b, base):
            self.zs[b] = self.pf[b].astype(BF16)
            far = 2 if b % 2 == 0 else 6
            for k, via, buf, n, sem in (
                (4, far, self.za, 2, self.za_r),
                (3, 1, self.za, 0, self.za_r),
                (5, 7, self.za, 1, self.za_r),
                (1, 1, self.zb, 0, self.zb_r),
                (7, 7, self.zb, 1, self.zb_r),
            ):
                src = self.zs.at[b, slot_of(k, base)]
                send(src, buf.at[b, n], self.z1_s, sem.at[b], dev(x, y, (z + via) % NZ, c))

        def z_second(self, b, base):
            arrived(self.za.at[b], self.za_r.at[b])
            for n, k in enumerate((2, 6)):
                part = self.pf[b, slot_of(k, base)] + self.za[b, n].astype(F32)
                if b % 2 == n:
                    part = part + self.za[b, 2].astype(F32)
                self.zt[b, n] = part.astype(BF16)
                there = dev(x, y, (z + k) % NZ, c)
                send(self.zt.at[b, n], self.zb.at[b, 2 + n], self.z2_s, self.zb_r.at[b], there)

        def y_share(self, b, base):
            arrived(self.zb.at[b], self.zb_r.at[b])
            slot = slot_of(0, base)
            total = self.pf[b, slot]
            for k in range(4):
                total = total + self.zb[b, k].astype(F32)
            self.pf[b, slot] = total
            self.ys[b] = total.astype(BF16)
            for k in range(1, NY):
                yc = (y + k) % NY
                send(self.ys.at[b, yc], self.yb.at[b, k - 1], self.y_s, self.yb_r.at[b], dev(x, yc, z, c))

        def home(self, b, base, own_plane, place):
            arrived(self.yb.at[b], self.yb_r.at[b])
            slot = slot_of(0, base)
            total = self.pf[b, slot, y]
            for k in range(3):
                total = total + self.yb[b, k].astype(F32)
            deliver(total, slot, self.out.at[b], self.f_s.at[b], base, own_plane, place)

        def ends(self, plan):
            arrived(self.zs.at[:, pl.ds(0, 5)], self.z1_s)
            arrived(self.zt, self.z2_s)
            arrived(self.yb, self.y_s)
            delivered(self.out, self.f_s, plan)

    def deliver(total, slot, out, sem, base, own_plane, place):
        zh_ = 2 * base + slot // 4
        dst = outb.at[place(slot % 4)]

        def put(ref):
            for n in range(total.shape[1] // 128):
                ref[n] = total[:, 128 * n : 128 * n + 128].astype(BF16)

        if own_plane:

            @pl.when(zh_ == z)
            def _():
                put(dst)

            @pl.when(zh_ != z)
            def _():
                put(out)
                send(out, dst, sem, f_r, dev(x, y, zh_, c))

        else:
            put(out)
            send(out, dst, sem, f_r, dev(xa, y, zh_, c))

    def delivered(out, sems, plan):
        for b, (base, own_plane, _) in enumerate(plan):
            if own_plane:

                @pl.when(2 * base + slot_of(0, base) // 4 != z)
                def _():
                    arrived(out.at[b], sems.at[b])

            else:
                arrived(out.at[b], sems.at[b])

    def slot_of(k, base):
        return (z + k - 2 * base + 3 + NZ) % NZ

    ysum, half, zsum = Sums(sums[:19]), Sums(sums[19:38]), SumsZ(sums[38:])

    def product(g, a, b):
        term = jnp.dot(gt[g].reshape(512, 1024), ab[a], preferred_element_type=F32)
        ysum.pf[b] = term.reshape(NY, 8, 16, 256)
        ysum.y_first(b)

    def product_half(g, t, b):
        right = ab[3, :, t * 128 : t * 128 + 128]
        term = jnp.dot(gt[g].reshape(512, 1024), right, preferred_element_type=F32)
        half.pf[b] = term.reshape(NY, 8, 16, 128)
        half.y_first(b)

    def product_z(g, a, b):
        term = jnp.dot(gt[g].reshape(512, 1024), ab[a], preferred_element_type=F32)
        term = term.reshape(NY, 8, 16, 256)
        for yc in range(NY):
            zsum.pf[b, :, yc] = term[yc]
        zsum.z_first(b, plan_z[b][0])

    def loop(count, fn):
        def step(t, _):
            fn(t)
            return 0

        lax.fori_loop(0, count, step, 0)

    def plan_of(pairs):
        def place(g, a):
            return lambda u: (g % 2 * 4 + u, pl.ds(a % 2 * 2, 2))

        return [(x if g < 2 else xg, a < 2, place(g, a)) for g, a in pairs]

    def half_place(g, t):
        return lambda u: (g % 2 * 4 + u, pl.ds(2 + t, 1))

    plan_y, plan_z = plan_of(PAIRS_Y), plan_of(PAIRS_Z)
    plan_half = [(x if g < 2 else xg, False, half_place(g, t)) for g, t in HALVES]

    def zf(*batches):
        for b in batches:
            ysum.z_first(b, plan_y[b][0])

    def zs(*batches):
        for b in batches:
            ysum.z_second(b, plan_y[b][0])

    def zh(*batches):
        for b in batches:
            ysum.home(b, *plan_y[b])

    def y2(*batches):
        for b in batches:
            ysum.y_second(b)

    def hf(*batches):
        for b in batches:
            half.z_first(b, plan_half[b][0])

    def hs(*batches):
        for b in batches:
            half.z_second(b, plan_half[b][0])

    def hh(*batches):
        for b in batches:
            half.home(b, *plan_half[b])

    def h2(*batches):
        for b in batches:
            half.y_second(b)

    def zz(b):
        zsum.z_second(b, plan_z[b][0])

    def zy(b):
        zsum.y_share(b, plan_z[b][0])

    def zn(b):
        zsum.home(b, *plan_z[b])

    def pass_on(j):
        src = gt.at[2 + j, :, c]
        arrived(src, gx_r.at[j])
        send(src, src, gf_s.at[j], gf_r.at[j], dev(x, y, z, 1 - c))

    def passed_on(j):
        arrived(gt.at[2 + j, :, 1 - c], gf_r.at[j])

    def coef_step(r, accs):
        rows = pl.ds(pl.multiple_of(r * 16, 16), 16)
        accs = list(accs)
        for q in range(4):
            cols = pl.ds(q * 128, 128)
            outs = [lo[j, rows, cols].astype(F32) for j in range(5)]
            grads = [ag[i, rows, cols].astype(F32) for i in range(4)]
            for n, (i, j) in enumerate(PAIRS):
                p = grads[i] * outs[j]
                accs[n] = accs[n] + (p[:8] + p[8:])
        return tuple(accs)

    def spread(buf, own, k0, targets, stage, size):
        for k, where in enumerate(targets):
            send(buf.at[own], buf.at[own], c_s.at[stage], c_r.at[stage], where)

    def settle(buf, own, stage, size):
        arrived(buf.at[pl.ds(0, size - 1)], c_r.at[stage])
        total = buf[0]
        for k in range(1, size):
            total = total + buf[k]
        return total

    def coef_local():
        for name in ["ag0", "ag1"] + [f"lo{j}" for j in range(5)]:
            loads[name].wait()
        zero = jnp.zeros((8, 128), F32)
        accs = lax.fori_loop(0, 64, coef_step, (zero,) * len(PAIRS))
        row = lax.broadcasted_iota(jnp.int32, (8, 128), 0)
        col = lax.broadcasted_iota(jnp.int32, (8, 128), 1)
        tile = zero
        for n, (i, j) in enumerate(PAIRS):
            total = jnp.sum(jnp.sum(accs[n], axis=0, keepdims=True), axis=1, keepdims=True)
            tile = jnp.where((row == i) & (col == j), jnp.broadcast_to(total, (8, 128)), tile)
        cb_c[c] = tile
        spread(cb_c, c, 0, [dev(x, y, z, 1 - c)], 0, 2)

    def coef_x():
        cb_x[x] = settle(cb_c, c, 0, 2)
        spread(cb_x, x, 0, [dev(x_, y, z, c) for x_ in others_x], 1, NX)

    def coef_y():
        cb_y[y] = settle(cb_x, x, 1, NX)
        spread(cb_y, y, 0, [dev(x, y_, z, c) for y_ in others_y], 2, NY)

    def coef_z():
        cb_z[z] = settle(cb_y, y, 2, NY)
        spread(cb_z, z, 0, [dev(x, y, z_, c) for z_ in others_z], 3, NZ)

    for j in range(2):
        arrived(gt.at[j, :, 1 - c], gd_r.at[j])
    product_z(1, 1, 0)
    loop(3, lambda t: product(t // 2, t % 2, t))
    y2(0, 1, 2)
    coef_local()
    zz(0)
    zf(0)

    arrived(ab_piece(2, 0), ax_r.at[0])
    pass_on(0)
    product_z(0, 2, 1)
    product_z(1, 2, 2)
    passed_on(0)
    product_z(2, 2, 3)
    loop(2, lambda t: product(2, t, 3 + t))
    zf(1, 2)
    zs(0)

    arrived(ab_piece(2, 1), ax_r.at[1])
    loop(3, lambda t: product_half(t, 0, t))
    coef_x()
    y2(3, 4)
    zy(0)
    zz(1)
    h2(0, 1, 2)
    zs(1, 2)
    zz(2)

    arrived(ab_piece(2, 2), ax_r.at[2])
    pass_on(1)
    loop(3, lambda t: product_half(t, 1, 3 + t))
    zf(3, 4)
    passed_on(1)
    product_z(3, 3, 4)
    loop(3, lambda t: product(3, 2 - t, 5 + t))
    coef_y()
    h2(3, 4, 5)
    zz(3)
    hf(0, 1)
    y2(5)
    hf(2)
    y2(6, 7)
    zs(3, 4)
    zh(0, 1, 2)
    zn(0)
    zy(1)
    zy(2)
    hf(3)
    zz(4)
    hf(4, 5)
    hs(0, 1, 2)
    coef_z()
    zf(5, 6, 7)
    hs(3, 4, 5)
    zh(3, 4)
    zs(5, 6)
    zy(3)
    zy(4)
    zs(7)
    hh(0, 1, 2, 3, 4, 5)
    zn(1)
    zn(2)
    coef_out[...] = settle(cb_z, z, 3, NZ)
    zh(5, 6)
    zn(3)
    zn(4)
    zh(7)

    at_home = z // 4 == x // 2

    @pl.when(at_home)
    def _():
        arrived(outb.at[pl.ds(0, 6)], f_r)

    @pl.when(jnp.logical_not(at_home))
    def _():
        arrived(outb, f_r)

    proj_out[...] = outb[...]

    ysum.ends(plan_y)
    half.ends(plan_half)
    zsum.ends(plan_z)
    arrived(cb_c.at[0], c_s.at[0])
    arrived(cb_x.at[pl.ds(0, NX - 1)], c_s.at[1])
    arrived(cb_y.at[pl.ds(0, NY - 1)], c_s.at[2])
    arrived(cb_z.at[pl.ds(0, NZ - 1)], c_s.at[3])
    for j in range(2):
        arrived(gt.at[j, :, c], gx_s.at[j])
        arrived(gt.at[j, :, c], gd_s.at[j])
        arrived(gt.at[2 + j, :, c], gf_s.at[j])
    for j in range(3):
        arrived(ab_piece(0, j), ax_s.at[j])


OUT_COEF, OUT_PROJ = pltpu.VMEM((8, 128), F32), pltpu.VMEM((8, 4, 16, 128), BF16)


def sums_scratch(count, width):
    dma = pltpu.SemaphoreType.DMA
    return [
        pltpu.VMEM((count, NY, 8, 16, width), F32),
        pltpu.VMEM((count, 2, 4, 16, width), BF16),
        pltpu.VMEM((count, 2, 4, 16, width), BF16),
        pltpu.VMEM((count, 2, 8, 16, width), BF16),
        pltpu.VMEM((count, 2, 8, 16, width), BF16),
        pltpu.VMEM((count, 8, 16, width), BF16),
        pltpu.VMEM((count, 3, 16, width), BF16),
        pltpu.VMEM((count, 2, 16, width), BF16),
        pltpu.VMEM((count, 4, 16, width), BF16),
        pltpu.VMEM((count, width // 128, 16, 128), BF16),
        dma(()), dma((count, 2)), dma(()), dma((count, 2)),
        dma(()), dma((count,)), dma(()), dma((count,)),
        dma((count,)),
    ]


def sums_z_scratch(count):
    dma = pltpu.SemaphoreType.DMA
    return [
        pltpu.VMEM((count, 8, NY, 16, 256), F32),
        pltpu.VMEM((count, 8, NY, 16, 256), BF16),
        pltpu.VMEM((count, 3, NY, 16, 256), BF16),
        pltpu.VMEM((count, 2, NY, 16, 256), BF16),
        pltpu.VMEM((count, 4, NY, 16, 256), BF16),
        pltpu.VMEM((count, NY, 16, 256), BF16),
        pltpu.VMEM((count, 3, 16, 256), BF16),
        pltpu.VMEM((count, 2, 16, 128), BF16),
        dma(()), dma((count,)), dma(()), dma((count,)),
        dma(()), dma((count,)), dma((count,)),
    ]


def local(layer_outs, avg_grads, attn_mixed, dwa_coefs):
    dma = pltpu.SemaphoreType.DMA
    anywhere = pl.BlockSpec(memory_space=pl.ANY)
    vmem = pl.BlockSpec(memory_space=pltpu.VMEM)
    coef, proj = pl.pallas_call(
        kernel,
        out_shape=(OUT_COEF, OUT_PROJ),
        in_specs=[pl.BlockSpec(memory_space=pltpu.SMEM), anywhere, anywhere, anywhere],
        out_specs=(vmem, vmem),
        scratch_shapes=[
            pltpu.VMEM((5, 1024, 512), BF16),
            pltpu.VMEM((4, 1024, 512), BF16),
            pltpu.VMEM((4, 1024, 256), BF16),
            pltpu.VMEM((4, NY, 2, 64, 1024), BF16),
            pltpu.VMEM((8, 4, 16, 128), BF16),
            pltpu.VMEM((2, 8, 128), F32),
            pltpu.VMEM((NX, 8, 128), F32),
            pltpu.VMEM((NY, 8, 128), F32),
            pltpu.VMEM((NZ, 8, 128), F32),
            dma((13,)),
            dma((2,)), dma((2,)), dma((2,)), dma((2,)),
            dma((2,)), dma((2,)), dma((3,)), dma((3,)),
            dma(()), dma((4,)), dma((4,)),
            *sums_scratch(len(PAIRS_Y), 256),
            *sums_scratch(len(HALVES), 128),
            *sums_z_scratch(len(PAIRS_Z)),
        ],
        compiler_params=pltpu.CompilerParams(
            collective_id=0, has_side_effects=True, vmem_limit_bytes=56 * 1024 * 1024
        ),
    )(dwa_coefs, layer_outs, avg_grads, attn_mixed)
    coef = pltpu.with_memory_space_constraint(coef, pltpu.VMEM)
    proj = pltpu.with_memory_space_constraint(proj, pltpu.VMEM)
    return pl.pallas_call(
        lay_out,
        out_shape=(jax.ShapeDtypeStruct((4, 5), F32), jax.ShapeDtypeStruct((128, 512), F32)),
        in_specs=[vmem, vmem],
        out_specs=(vmem, vmem),
    )(coef, proj)


def lay_out(coef, proj, coef_out, proj_out):
    coef_out[...] = coef[:4, :5]
    for block in range(8):
        for j in range(4):
            proj_out[pl.ds(block * 16, 16), pl.ds(j * 128, 128)] = proj[block, j].astype(F32)


def solution(mesh):
    in_specs = (P(None, "dp", "tensor"), P(None, "dp", "tensor"), P("dp", "tensor"), P())
    out_specs = (P(), P("dp", "tensor"))
    return jax.shard_map(local, mesh=mesh, in_specs=in_specs, out_specs=out_specs, check_vma=False)
```

```python
import jax
import jax.numpy as jnp
from jax import lax
from jax.experimental import pallas as pl
from jax.experimental.pallas import tpu as pltpu
from jax.sharding import PartitionSpec as P

MESH = pl.DeviceIdType.MESH
F32, BF16 = jnp.float32, jnp.bfloat16
NX, NY, NZ = 4, 4, 8
PAIRS_Z = [(1, 1), (0, 2), (1, 2), (2, 2), (3, 3)]
PAIRS_Y = [(0, 0), (0, 1), (1, 0), (2, 0), (2, 1), (3, 2), (3, 1), (3, 0)]
HALVES = [(g, t) for t in range(2) for g in range(3)]
PAIRS = [(i, j) for i in range(4) for j in range(5) if j <= i + 1]


def kernel(
    co, lo_h, ag_h, at_h, coef_out, proj_out,
    lo, ag, ab, gt, outb, cb_c, cb_x, cb_y, cb_z,
    in_sem, gd_s, gd_r, gx_s, gx_r, gf_s, gf_r, ax_s, ax_r, f_r, c_s, c_r,
    *sums,
):
    dp, tk = lax.axis_index("dp"), lax.axis_index("tensor")
    z, y = dp // NY, dp % NY
    x, c = tk // 2, tk % 2
    xg = x + 1 - 2 * (x % 2)
    xa = NX - 1 - x

    def dev(x_, y_, z_, c_):
        return (z_ * NY + y_, x_ * 2 + c_)

    def send(src, dst, send_sem, recv_sem, where):
        copy = pltpu.make_async_remote_copy(
            src_ref=src, dst_ref=dst, send_sem=send_sem, recv_sem=recv_sem,
            device_id=where, device_id_type=MESH,
        )
        copy.start()

    def arrived(ref, sem):
        pltpu.make_async_copy(ref, ref, sem).wait()

    others_x = [(x + k) % NX for k in range(1, NX)]
    others_y = [(y + k) % NY for k in range(1, NY)]
    others_z = [(z + k) % NZ for k in range(1, NZ)]

    loads = {}

    def load(name, src, dst, i):
        loads[name] = pltpu.make_async_copy(src, dst, in_sem.at[i])
        loads[name].start()

    for part in range(2):
        rows = pl.ds(part * 512, 512)
        load(f"ag2{part}", ag_h.at[2, rows], ag.at[2, rows], part)
        load(f"ag3{part}", ag_h.at[3, rows], ag.at[3, rows], 11 + part)
    load("ab0", at_h.at[:, pl.ds(0, 256)], ab.at[0], 2)
    load("ab1", at_h.at[:, pl.ds(256, 256)], ab.at[1], 3)
    load("ag0", ag_h.at[0], ag.at[0], 4)
    load("ag1", ag_h.at[1], ag.at[1], 5)
    for j in range(5):
        load(f"lo{j}", lo_h.at[j], lo.at[j], 6 + j)

    barrier = pltpu.get_barrier_semaphore()
    greeted = [dev(x, y, z, 1 - c)]
    greeted += [dev(x_, y, z, c) for x_ in others_x]
    greeted += [dev(x, y_, z, c) for y_ in others_y]
    greeted += [dev(x, y, z_, c) for z_ in others_z]
    greeted += [dev(xa, y, z_, c) for z_ in others_z]
    for where in greeted:
        pl.semaphore_signal(barrier, inc=1, device_id=where, device_id_type=MESH)

    def ab_piece(n, j):
        return ab.at[n] if j == 0 else ab.at[n + 1, :, pl.ds(128 * (j - 1), 128)]

    c2, c3 = co[2, 3], co[3, 3]

    def out_grad(i, _):
        rows = pl.ds(pl.multiple_of(i * 256, 256), 256)
        for yy in range(NY):
            cols = pl.ds(yy * 128, 128)
            first = c2 * ag[2, rows, cols].astype(F32)
            second = c3 * ag[3, rows, cols].astype(F32)
            turned = (first + second).astype(BF16).T
            for hh in range(2):
                gt[hh, yy, c, :, rows] = turned[hh * 64 : hh * 64 + 64]
        return 0

    for part in range(2):
        loads[f"ag2{part}"].wait()
        loads[f"ag3{part}"].wait()
        lax.fori_loop(2 * part, 2 * part + 2, out_grad, 0)
    pl.semaphore_wait(barrier, len(greeted))
    for j in range(2):
        send(gt.at[j, :, c], gt.at[j, :, c], gd_s.at[j], gd_r.at[j], dev(x, y, z, 1 - c))
        send(gt.at[j, :, c], gt.at[2 + j, :, c], gx_s.at[j], gx_r.at[j], dev(xg, y, z, c))
        loads[f"ab{j}"].wait()
        for n in ((0,), (1, 2))[j]:
            send(ab_piece(0, n), ab_piece(2, n), ax_s.at[n], ax_r.at[n], dev(xa, y, z, c))

    up, down = dev(x, (y + 1) % NY, z, c), dev(x, (y + 3) % NY, z, c)

    class Sums:
        def __init__(self, refs, direct=()):
            self.direct = direct
            (
                self.pf, self.s1, self.r1, self.s2, self.r2, self.zs, self.za, self.zt, self.zb,
                self.out, self.y1_s, self.y1_r, self.y2_s, self.y2_r, self.z1_s, self.za_r,
                self.z2_s, self.zb_r, self.f_s,
            ) = refs

        def y_first(self, b):
            far = self.pf[b, (y + 2) % NY].astype(BF16)
            for i, where in enumerate((up, down)):
                self.s1[b, i] = far[4 * i : 4 * i + 4]
                send(self.s1.at[b, i], self.r1.at[b, i], self.y1_s, self.y1_r.at[b, i], where)

        def y_second(self, b):
            for i, (where, yc) in enumerate(((up, (y + 1) % NY), (down, (y + 3) % NY))):
                arrived(self.r1.at[b, i], self.y1_r.at[b, i])
                both, alone = pl.ds(4 * i, 4), pl.ds(4 - 4 * i, 4)
                self.s2[b, i, both] = (self.pf[b, yc, both] + self.r1[b, i].astype(F32)).astype(BF16)
                self.s2[b, i, alone] = self.pf[b, yc, alone].astype(BF16)
                send(self.s2.at[b, i], self.r2.at[b, i], self.y2_s, self.y2_r.at[b, i], where)

        def z_first(self, b, base):
            arrived(self.r2.at[b, 0], self.y2_r.at[b, 0])
            arrived(self.r2.at[b, 1], self.y2_r.at[b, 1])
            total = self.pf[b, y] + self.r2[b, 0].astype(F32) + self.r2[b, 1].astype(F32)
            self.pf[b, y] = total
            self.zs[b] = total.astype(BF16)
            far = 2 if b % 2 == 0 else 6
            steps = [
                (4, far, self.za, 2, self.za_r),
                (3, 1, self.za, 0, self.za_r),
                (5, 7, self.za, 1, self.za_r),
                (1, 1, self.zb, 0, self.zb_r),
                (7, 7, self.zb, 1, self.zb_r),
            ]
            if b in self.direct:
                steps = [(k, k, buf, n, sem) for k, _, buf, n, sem in steps]
                steps += [(2, 2, self.zb, 2, self.zb_r), (6, 6, self.zb, 3, self.zb_r)]
            for i, (k, via, buf, n, sem) in enumerate(steps):
                src = self.zs.at[b, slot_of(k, base)]
                gone = self.z1_s if i < 5 else self.z2_s
                send(src, buf.at[b, n], gone, sem.at[b], dev(x, y, (z + via) % NZ, c))

        def z_second(self, b, base):
            if b in self.direct:
                return
            arrived(self.za.at[b], self.za_r.at[b])
            for n, k in enumerate((2, 6)):
                part = self.pf[b, y, slot_of(k, base)] + self.za[b, n].astype(F32)
                if b % 2 == n:
                    part = part + self.za[b, 2].astype(F32)
                self.zt[b, n] = part.astype(BF16)
                there = dev(x, y, (z + k) % NZ, c)
                send(self.zt.at[b, n], self.zb.at[b, 2 + n], self.z2_s, self.zb_r.at[b], there)

        def home(self, b, base, own_plane, place):
            arrived(self.zb.at[b], self.zb_r.at[b])
            slot = slot_of(0, base)
            total = self.pf[b, y, slot]
            for k in range(4):
                total = total + self.zb[b, k].astype(F32)
            if b in self.direct:
                arrived(self.za.at[b], self.za_r.at[b])
                for k in range(3):
                    total = total + self.za[b, k].astype(F32)
            deliver(total, slot, self.out.at[b], self.f_s.at[b], base, own_plane, place)

        def ends(self, plan):
            arrived(self.s1, self.y1_s)
            arrived(self.s2, self.y2_s)
            arrived(self.zs.at[:, pl.ds(0, 5)], self.z1_s)
            arrived(self.zt, self.z2_s)
            delivered(self.out, self.f_s, plan)

    class SumsZ:
        def __init__(self, refs):
            (
                self.pf, self.zs, self.za, self.zt, self.zb, self.ys, self.yb, self.out,
                self.z1_s, self.za_r, self.z2_s, self.zb_r, self.y_s, self.yb_r, self.f_s,
            ) = refs

        def z_first(self, b, base):
            self.zs[b] = self.pf[b].astype(BF16)
            far = 2 if b % 2 == 0 else 6
            for k, via, buf, n, sem in (
                (4, far, self.za, 2, self.za_r),
                (3, 1, self.za, 0, self.za_r),
                (5, 7, self.za, 1, self.za_r),
                (1, 1, self.zb, 0, self.zb_r),
                (7, 7, self.zb, 1, self.zb_r),
            ):
                src = self.zs.at[b, slot_of(k, base)]
                send(src, buf.at[b, n], self.z1_s, sem.at[b], dev(x, y, (z + via) % NZ, c))

        def z_second(self, b, base):
            arrived(self.za.at[b], self.za_r.at[b])
            for n, k in enumerate((2, 6)):
                part = self.pf[b, slot_of(k, base)] + self.za[b, n].astype(F32)
                if b % 2 == n:
                    part = part + self.za[b, 2].astype(F32)
                self.zt[b, n] = part.astype(BF16)
                there = dev(x, y, (z + k) % NZ, c)
                send(self.zt.at[b, n], self.zb.at[b, 2 + n], self.z2_s, self.zb_r.at[b], there)

        def y_share(self, b, base):
            arrived(self.zb.at[b], self.zb_r.at[b])
            slot = slot_of(0, base)
            total = self.pf[b, slot]
            for k in range(4):
                total = total + self.zb[b, k].astype(F32)
            self.pf[b, slot] = total
            self.ys[b] = total.astype(BF16)
            for k in range(1, NY):
                yc = (y + k) % NY
                send(self.ys.at[b, yc], self.yb.at[b, k - 1], self.y_s, self.yb_r.at[b], dev(x, yc, z, c))

        def home(self, b, base, own_plane, place):
            arrived(self.yb.at[b], self.yb_r.at[b])
            slot = slot_of(0, base)
            total = self.pf[b, slot, y]
            for k in range(3):
                total = total + self.yb[b, k].astype(F32)
            deliver(total, slot, self.out.at[b], self.f_s.at[b], base, own_plane, place)

        def ends(self, plan):
            arrived(self.zs.at[:, pl.ds(0, 5)], self.z1_s)
            arrived(self.zt, self.z2_s)
            arrived(self.yb, self.y_s)
            delivered(self.out, self.f_s, plan)

    def deliver(total, slot, out, sem, base, own_plane, place):
        zh_ = 2 * base + slot // 4
        dst = outb.at[place(slot % 4)]

        def put(ref):
            for n in range(total.shape[1] // 128):
                ref[n] = total[:, 128 * n : 128 * n + 128].astype(BF16)

        if own_plane:

            @pl.when(zh_ == z)
            def _():
                put(dst)

            @pl.when(zh_ != z)
            def _():
                put(out)
                send(out, dst, sem, f_r, dev(x, y, zh_, c))

        else:
            put(out)
            send(out, dst, sem, f_r, dev(xa, y, zh_, c))

    def delivered(out, sems, plan):
        for b, (base, own_plane, _) in enumerate(plan):
            if own_plane:

                @pl.when(2 * base + slot_of(0, base) // 4 != z)
                def _():
                    arrived(out.at[b], sems.at[b])

            else:
                arrived(out.at[b], sems.at[b])

    def slot_of(k, base):
        return (z + k - 2 * base + 3 + NZ) % NZ

    ysum, half, zsum = Sums(sums[:19], (5, 6, 7)), Sums(sums[19:38]), SumsZ(sums[38:])

    def product(g, a, b):
        term = jnp.dot(gt[g].reshape(512, 1024), ab[a], preferred_element_type=F32)
        ysum.pf[b] = term.reshape(NY, 8, 16, 256)
        ysum.y_first(b)

    def product_half(g, t, b):
        right = ab[3, :, t * 128 : t * 128 + 128]
        term = jnp.dot(gt[g].reshape(512, 1024), right, preferred_element_type=F32)
        half.pf[b] = term.reshape(NY, 8, 16, 128)
        half.y_first(b)

    def product_z(g, a, b):
        term = jnp.dot(gt[g].reshape(512, 1024), ab[a], preferred_element_type=F32)
        term = term.reshape(NY, 8, 16, 256)
        for yc in range(NY):
            zsum.pf[b, :, yc] = term[yc]
        zsum.z_first(b, plan_z[b][0])

    def loop(count, fn):
        def step(t, _):
            fn(t)
            return 0

        lax.fori_loop(0, count, step, 0)

    def plan_of(pairs):
        def place(g, a):
            return lambda u: (g % 2 * 4 + u, pl.ds(a % 2 * 2, 2))

        return [(x if g < 2 else xg, a < 2, place(g, a)) for g, a in pairs]

    def half_place(g, t):
        return lambda u: (g % 2 * 4 + u, pl.ds(2 + t, 1))

    plan_y, plan_z = plan_of(PAIRS_Y), plan_of(PAIRS_Z)
    plan_half = [(x if g < 2 else xg, False, half_place(g, t)) for g, t in HALVES]

    def zf(*batches):
        for b in batches:
            ysum.z_first(b, plan_y[b][0])

    def zs(*batches):
        for b in batches:
            ysum.z_second(b, plan_y[b][0])

    def zh(*batches):
        for b in batches:
            ysum.home(b, *plan_y[b])

    def y2(*batches):
        for b in batches:
            ysum.y_second(b)

    def hf(*batches):
        for b in batches:
            half.z_first(b, plan_half[b][0])

    def hs(*batches):
        for b in batches:
            half.z_second(b, plan_half[b][0])

    def hh(*batches):
        for b in batches:
            half.home(b, *plan_half[b])

    def h2(*batches):
        for b in batches:
            half.y_second(b)

    def zz(b):
        zsum.z_second(b, plan_z[b][0])

    def zy(b):
        zsum.y_share(b, plan_z[b][0])

    def zn(b):
        zsum.home(b, *plan_z[b])

    def pass_on(j):
        src = gt.at[2 + j, :, c]
        arrived(src, gx_r.at[j])
        send(src, src, gf_s.at[j], gf_r.at[j], dev(x, y, z, 1 - c))

    def passed_on(j):
        arrived(gt.at[2 + j, :, 1 - c], gf_r.at[j])

    def coef_step(r, accs):
        rows = pl.ds(pl.multiple_of(r * 16, 16), 16)
        accs = list(accs)
        for q in range(4):
            cols = pl.ds(q * 128, 128)
            outs = [lo[j, rows, cols].astype(F32) for j in range(5)]
            grads = [ag[i, rows, cols].astype(F32) for i in range(4)]
            for n, (i, j) in enumerate(PAIRS):
                p = grads[i] * outs[j]
                accs[n] = accs[n] + (p[:8] + p[8:])
        return tuple(accs)

    def spread(buf, own, k0, targets, stage, size):
        for k, where in enumerate(targets):
            send(buf.at[own], buf.at[own], c_s.at[stage], c_r.at[stage], where)

    def settle(buf, own, stage, size):
        arrived(buf.at[pl.ds(0, size - 1)], c_r.at[stage])
        total = buf[0]
        for k in range(1, size):
            total = total + buf[k]
        return total

    def coef_local():
        for name in ["ag0", "ag1"] + [f"lo{j}" for j in range(5)]:
            loads[name].wait()
        zero = jnp.zeros((8, 128), F32)
        accs = lax.fori_loop(0, 64, coef_step, (zero,) * len(PAIRS))
        row = lax.broadcasted_iota(jnp.int32, (8, 128), 0)
        col = lax.broadcasted_iota(jnp.int32, (8, 128), 1)
        tile = zero
        for n, (i, j) in enumerate(PAIRS):
            total = jnp.sum(jnp.sum(accs[n], axis=0, keepdims=True), axis=1, keepdims=True)
            tile = jnp.where((row == i) & (col == j), jnp.broadcast_to(total, (8, 128)), tile)
        cb_c[c] = tile
        spread(cb_c, c, 0, [dev(x, y, z, 1 - c)], 0, 2)

    def coef_x():
        cb_x[x] = settle(cb_c, c, 0, 2)
        spread(cb_x, x, 0, [dev(x_, y, z, c) for x_ in others_x], 1, NX)

    def coef_y():
        cb_y[y] = settle(cb_x, x, 1, NX)
        spread(cb_y, y, 0, [dev(x, y_, z, c) for y_ in others_y], 2, NY)

    def coef_z():
        cb_z[z] = settle(cb_y, y, 2, NY)
        spread(cb_z, z, 0, [dev(x, y, z_, c) for z_ in others_z], 3, NZ)

    for j in range(2):
        arrived(gt.at[j, :, 1 - c], gd_r.at[j])
    product_z(1, 1, 0)
    loop(3, lambda t: product(t // 2, t % 2, t))
    y2(0, 1, 2)
    coef_local()
    zz(0)
    zf(0)

    arrived(ab_piece(2, 0), ax_r.at[0])
    pass_on(0)
    product_z(0, 2, 1)
    product_z(1, 2, 2)
    passed_on(0)
    product_z(2, 2, 3)
    loop(2, lambda t: product(2, t, 3 + t))
    zf(1, 2)
    zs(0)

    arrived(ab_piece(2, 1), ax_r.at[1])
    loop(3, lambda t: product_half(t, 0, t))
    coef_x()
    y2(3, 4)
    zy(0)
    zz(1)
    h2(0, 1, 2)
    zs(1, 2)
    zz(2)

    arrived(ab_piece(2, 2), ax_r.at[2])
    pass_on(1)
    loop(3, lambda t: product_half(t, 1, 3 + t))
    zf(3, 4)
    passed_on(1)
    product_z(3, 3, 4)
    loop(3, lambda t: product(3, 2 - t, 5 + t))
    coef_y()
    h2(3, 4, 5)
    zz(3)
    hf(0, 1)
    y2(5)
    hf(2)
    y2(6, 7)
    zs(3, 4)
    zh(0, 1, 2)
    zn(0)
    zy(1)
    zy(2)
    hf(3)
    zz(4)
    hf(4, 5)
    hs(0, 1, 2)
    coef_z()
    zf(5, 6, 7)
    hs(3, 4, 5)
    zh(3, 4)
    zs(5, 6)
    zy(3)
    zy(4)
    zs(7)
    hh(0, 1, 2, 3, 4, 5)
    zn(1)
    zn(2)
    coef_out[...] = settle(cb_z, z, 3, NZ)
    zh(5, 6)
    zn(3)
    zn(4)
    zh(7)

    at_home = z // 4 == x // 2

    @pl.when(at_home)
    def _():
        arrived(outb.at[pl.ds(0, 6)], f_r)

    @pl.when(jnp.logical_not(at_home))
    def _():
        arrived(outb, f_r)

    proj_out[...] = outb[...]

    ysum.ends(plan_y)
    half.ends(plan_half)
    zsum.ends(plan_z)
    arrived(cb_c.at[0], c_s.at[0])
    arrived(cb_x.at[pl.ds(0, NX - 1)], c_s.at[1])
    arrived(cb_y.at[pl.ds(0, NY - 1)], c_s.at[2])
    arrived(cb_z.at[pl.ds(0, NZ - 1)], c_s.at[3])
    for j in range(2):
        arrived(gt.at[j, :, c], gx_s.at[j])
        arrived(gt.at[j, :, c], gd_s.at[j])
        arrived(gt.at[2 + j, :, c], gf_s.at[j])
    for j in range(3):
        arrived(ab_piece(0, j), ax_s.at[j])


OUT_COEF, OUT_PROJ = pltpu.VMEM((8, 128), F32), pltpu.VMEM((8, 4, 16, 128), BF16)


def sums_scratch(count, width):
    dma = pltpu.SemaphoreType.DMA
    return [
        pltpu.VMEM((count, NY, 8, 16, width), F32),
        pltpu.VMEM((count, 2, 4, 16, width), BF16),
        pltpu.VMEM((count, 2, 4, 16, width), BF16),
        pltpu.VMEM((count, 2, 8, 16, width), BF16),
        pltpu.VMEM((count, 2, 8, 16, width), BF16),
        pltpu.VMEM((count, 8, 16, width), BF16),
        pltpu.VMEM((count, 3, 16, width), BF16),
        pltpu.VMEM((count, 2, 16, width), BF16),
        pltpu.VMEM((count, 4, 16, width), BF16),
        pltpu.VMEM((count, width // 128, 16, 128), BF16),
        dma(()), dma((count, 2)), dma(()), dma((count, 2)),
        dma(()), dma((count,)), dma(()), dma((count,)),
        dma((count,)),
    ]


def sums_z_scratch(count):
    dma = pltpu.SemaphoreType.DMA
    return [
        pltpu.VMEM((count, 8, NY, 16, 256), F32),
        pltpu.VMEM((count, 8, NY, 16, 256), BF16),
        pltpu.VMEM((count, 3, NY, 16, 256), BF16),
        pltpu.VMEM((count, 2, NY, 16, 256), BF16),
        pltpu.VMEM((count, 4, NY, 16, 256), BF16),
        pltpu.VMEM((count, NY, 16, 256), BF16),
        pltpu.VMEM((count, 3, 16, 256), BF16),
        pltpu.VMEM((count, 2, 16, 128), BF16),
        dma(()), dma((count,)), dma(()), dma((count,)),
        dma(()), dma((count,)), dma((count,)),
    ]


def local(layer_outs, avg_grads, attn_mixed, dwa_coefs):
    dma = pltpu.SemaphoreType.DMA
    anywhere = pl.BlockSpec(memory_space=pl.ANY)
    vmem = pl.BlockSpec(memory_space=pltpu.VMEM)
    coef, proj = pl.pallas_call(
        kernel,
        out_shape=(OUT_COEF, OUT_PROJ),
        in_specs=[pl.BlockSpec(memory_space=pltpu.SMEM), anywhere, anywhere, anywhere],
        out_specs=(vmem, vmem),
        scratch_shapes=[
            pltpu.VMEM((5, 1024, 512), BF16),
            pltpu.VMEM((4, 1024, 512), BF16),
            pltpu.VMEM((4, 1024, 256), BF16),
            pltpu.VMEM((4, NY, 2, 64, 1024), BF16),
            pltpu.VMEM((8, 4, 16, 128), BF16),
            pltpu.VMEM((2, 8, 128), F32),
            pltpu.VMEM((NX, 8, 128), F32),
            pltpu.VMEM((NY, 8, 128), F32),
            pltpu.VMEM((NZ, 8, 128), F32),
            dma((13,)),
            dma((2,)), dma((2,)), dma((2,)), dma((2,)),
            dma((2,)), dma((2,)), dma((3,)), dma((3,)),
            dma(()), dma((4,)), dma((4,)),
            *sums_scratch(len(PAIRS_Y), 256),
            *sums_scratch(len(HALVES), 128),
            *sums_z_scratch(len(PAIRS_Z)),
        ],
        compiler_params=pltpu.CompilerParams(
            collective_id=0, has_side_effects=True, vmem_limit_bytes=56 * 1024 * 1024
        ),
    )(dwa_coefs, layer_outs, avg_grads, attn_mixed)
    coef = pltpu.with_memory_space_constraint(coef, pltpu.VMEM)
    proj = pltpu.with_memory_space_constraint(proj, pltpu.VMEM)
    return pl.pallas_call(
        lay_out,
        out_shape=(jax.ShapeDtypeStruct((4, 5), F32), jax.ShapeDtypeStruct((128, 512), F32)),
        in_specs=[vmem, vmem],
        out_specs=(vmem, vmem),
    )(coef, proj)


def lay_out(coef, proj, coef_out, proj_out):
    coef_out[...] = coef[:4, :5]
    for block in range(8):
        for j in range(4):
            proj_out[pl.ds(block * 16, 16), pl.ds(j * 128, 128)] = proj[block, j].astype(F32)


def solution(mesh):
    in_specs = (P(None, "dp", "tensor"), P(None, "dp", "tensor"), P("dp", "tensor"), P())
    out_specs = (P(), P("dp", "tensor"))
    return jax.shard_map(local, mesh=mesh, in_specs=in_specs, out_specs=out_specs, check_vma=False)
```
